32 devices in a mesh: cp: 32 (over z, y, x, core).
Axes of the slice: x: 2, y: 2, z: 4, core: 2. Of those that a mesh axis runs over, the one named last changes fastest.
Arguments:
- x_seq: bfloat16 [1, 24576, 80, 64], P(None, 'cp')
- dt_seq: float32 [1, 24576, 80], P(None, 'cp')
- a_log: float32 [80], replicated
- b_proj: bfloat16 [1, 24576, 128], P(None, 'cp')
- c_proj: bfloat16 [1, 24576, 128], P(None, 'cp')
- d_skip: float32 [80], replicated
- s_init: float32 [1, 80, 64, 128], replicated
- dy_seq: bfloat16 [1, 24576, 80, 64], P(None, 'cp')
- ds_last: float32 [1, 80, 64, 128], replicated
Outputs:
- output 1: bfloat16 [1, 24576, 80, 64], P(None, 'cp')
- output 2: float32 [1, 24576, 80], P(None, 'cp')
- output 3: bfloat16 [1, 24576, 128], P(None, 'cp')
- output 4: bfloat16 [1, 24576, 128], P(None, 'cp')
- output 5: float32 [1, 80, 64, 128], replicated
- output 6: float32 [80], replicated
- output 7: float32 [80], replicated
All inputs are finite; a program needn't handle non-finite values.
Results may differ from the reference program's by a relative error of at most 0.001.
Values sent between devices are 32-bit elements.
A program may use at most 1 GiB of HBM per device.

```python
import functools
import math
import jax
import jax.numpy as jnp
from jax import lax

BATCH = 1
SEQ = 24576
HEADS = 80
HEAD_DIM = 64
STATE = 128
CHUNK = 256
SPAN_LEN = 768


def setup_inputs(seed: int = 0) -> dict:
    rng_keys = jax.random.split(jax.random.key(seed), 10)
    x_seq = jax.random.normal(rng_keys[0], (BATCH, SEQ, HEADS, HEAD_DIM), jnp.float32).astype(jnp.bfloat16)
    dt_seq = jax.nn.softplus(0.5 * jax.random.normal(rng_keys[1], (BATCH, SEQ, HEADS), jnp.float32)) * (1.7 / SPAN_LEN)
    a_log = jax.random.uniform(rng_keys[2], (HEADS,), jnp.float32, math.log(0.25), 0.0)
    b_proj = jax.random.normal(rng_keys[3], (BATCH, SEQ, STATE), jnp.float32).astype(jnp.bfloat16)
    c_proj = jax.random.normal(rng_keys[4], (BATCH, SEQ, STATE), jnp.float32).astype(jnp.bfloat16)
    d_skip = jax.random.uniform(rng_keys[5], (HEADS,), jnp.float32, 0.2, 0.6)
    s_init = jax.random.normal(rng_keys[6], (BATCH, HEADS, HEAD_DIM, STATE), jnp.float32) * (SPAN_LEN ** -0.5)
    row_scale = jax.random.uniform(rng_keys[7], (BATCH, SEQ, 1, 1), jnp.float32, 0.5, 1.5)
    dy_seq = (jax.random.normal(rng_keys[8], (BATCH, SEQ, HEADS, HEAD_DIM), jnp.float32) * row_scale).astype(jnp.bfloat16)
    ds_last = jax.random.normal(rng_keys[9], (BATCH, HEADS, HEAD_DIM, STATE), jnp.float32) * (0.7 * SPAN_LEN ** 0.5)
    return {'x_seq': x_seq, 'dt_seq': dt_seq, 'a_log': a_log, 'b_proj': b_proj, 'c_proj': c_proj, 'd_skip': d_skip, 's_init': s_init, 'dy_seq': dy_seq, 'ds_last': ds_last}


def chunk_step(carry_state, blk_in, neg_rate, d_skip):
    x_blk, dt_blk, b_blk, c_blk = blk_in
    cum_decay = jnp.cumsum(dt_blk * neg_rate, axis=1)
    u_blk = x_blk * dt_blk[..., None]
    gram_mat = jnp.einsum('btn,bsn->bts', c_blk, b_blk)
    blk_len = x_blk.shape[1]
    causal = (jnp.arange(blk_len)[:, None] >= jnp.arange(blk_len)[None, :])[None, :, :, None]
    log_diff = jnp.where(causal, cum_decay[:, :, None, :] - cum_decay[:, None, :, :], 0.0)
    mix_mat = jnp.where(causal, jnp.exp(log_diff), 0.0) * gram_mat[..., None]
    y_blk = jnp.einsum('btsh,bshp->bthp', mix_mat, u_blk)
    y_blk = y_blk + jnp.exp(cum_decay)[..., None] * jnp.einsum('bhpn,btn->bthp', carry_state, c_blk)
    y_blk = y_blk + d_skip[:, None] * x_blk
    tail_decay = jnp.exp(cum_decay[:, -1:, :] - cum_decay)
    new_state = jnp.exp(cum_decay[:, -1, :])[..., None, None] * carry_state + jnp.einsum('bsh,bshp,bsn->bhpn', tail_decay, u_blk, b_blk)
    return new_state, y_blk


def ssd_forward(x_seq, dt_seq, a_log, b_proj, c_proj, d_skip, s_init):
    n_batch = x_seq.shape[0]
    n_span = SEQ // SPAN_LEN
    per_span = SPAN_LEN // CHUNK
    neg_rate = -jnp.exp(a_log)
    inner_step = jax.checkpoint(functools.partial(chunk_step, neg_rate=neg_rate, d_skip=d_skip))

    def span_step(carry_state, span_in):
        return lax.scan(inner_step, carry_state, span_in)

    def split_seq(array_in):
        blocks = array_in.astype(jnp.float32).reshape((n_batch, n_span, per_span, CHUNK) + array_in.shape[2:])
        return jnp.moveaxis(blocks, 0, 2)

    seq_in = (split_seq(x_seq), split_seq(dt_seq), split_seq(b_proj), split_seq(c_proj))
    final_state, y_blocks = lax.scan(jax.checkpoint(span_step), s_init, seq_in)
    y_seq = jnp.moveaxis(y_blocks, 2, 0).reshape(x_seq.shape)
    return y_seq, final_state


def reference(x_seq, dt_seq, a_log, b_proj, c_proj, d_skip, s_init, dy_seq, ds_last):
    _, pull_back = jax.vjp(ssd_forward, x_seq, dt_seq, a_log, b_proj, c_proj, d_skip, s_init)
    grad_x, grad_dt, grad_alog, grad_b, grad_c, grad_skip, grad_init = pull_back((dy_seq.astype(jnp.float32), ds_last))
    return (grad_x, grad_dt, grad_b, grad_c, grad_init, grad_alog, grad_skip)
```

```python
import functools
import jax
import jax.numpy as jnp
from jax import lax
from jax.experimental import pallas as pl
from jax.experimental.pallas import tpu as pltpu
from jax.sharding import PartitionSpec as P

AXIS = 'cp'
H, PD, N = 80, 64, 128
L = 128
HG = 8
LOG2E = 1.4426950408889634
NEG = -1e30
F32, BF16 = jnp.float32, jnp.bfloat16
HIGHEST = lax.Precision.HIGHEST
NT = (((1,), (1,)), ((), ()))
TN = (((0,), (0,)), ((), ()))
NN = (((1,), (0,)), ((), ()))


def dot(a, b, dims=NN, precision=None):
    return lax.dot_general(a, b, dims, precision=precision, preferred_element_type=F32)


def split(v):
    hi = v.astype(BF16)
    return hi, (v - hi.astype(F32)).astype(BF16)


MESH = pl.DeviceIdType.MESH


def greet_all(nd, me):
    barrier = pltpu.get_barrier_semaphore()
    for o in range(1, nd):
        pl.semaphore_signal(barrier, inc=1, device_id=(lax.rem(me + o, nd),), device_id_type=MESH)
    pl.semaphore_wait(barrier, nd - 1)


def tile_copy(nd, me, o, got, send, recv):
    return pltpu.make_async_remote_copy(src_ref=got.at[me], dst_ref=got.at[me], send_sem=send.at[o], recv_sem=recv.at[o],
                                        device_id=(lax.rem(me + o, nd),), device_id_type=MESH)


def send_all(nd, me, got, send, recv):
    for o in range(1, nd):
        tile_copy(nd, me, o, got, send, recv).start()


def wait_all(nd, me, got, send, recv):
    for o in range(1, nd):
        src = lax.rem(me + nd - o, nd)
        pltpu.make_async_remote_copy(src_ref=got.at[src], dst_ref=got.at[src], send_sem=send.at[o], recv_sem=recv.at[o],
                                     device_id=(src,), device_id_type=MESH).wait_recv()
        tile_copy(nd, me, o, got, send, recv).wait_send()


def summary_kernel(nd, x_ref, dy_ref, dt_ref, par_ref, b_ref, c_ref, s_ref, g_ref, cs_ref, tot_ref, all_ref,
                   tu_hi, tu_lo, sd_hi, sd_lo, cs_all, off_all, got, send, recv):
    nb = x_ref.shape[2] // L
    g = pl.program_id(0)
    me = lax.axis_index(AXIS)

    @pl.when(g == 0)
    def _():
        tri = (lax.broadcasted_iota(jnp.int32, (L, L), 0) <= lax.broadcasted_iota(jnp.int32, (L, L), 1)).astype(F32)
        off = jnp.zeros((H, L), F32)
        for b in range(nb):
            sl = slice(b * L, (b + 1) * L)
            a = dt_ref[:, sl] * (par_ref[:, 0:1] * LOG2E)
            cs = dot(a, tri, precision=HIGHEST)
            cs_all[:, sl] = cs
            off_all[:, sl] = off
            off = off + jnp.broadcast_to(cs[:, L - 1:L], (H, L))
        off_all[:, nb * L:] = off
        cs_ref[...] = cs_all[...]
        tot_ref[...] = off
        got[me] = jnp.transpose(jnp.concatenate([off, jnp.zeros((L - H, L), F32)], axis=0))[:8]
        greet_all(nd, me)
        send_all(nd, me, got, send, recv)

    rows = pl.ds(pl.multiple_of(g * HG, HG), HG)
    for b in range(nb):
        sl = slice(b * L, (b + 1) * L)
        run = cs_all[rows, sl] + off_all[rows, sl]
        ec = jnp.exp2(run)
        tl = jnp.exp2(off_all[rows, nb * L:] - run) * dt_ref[rows, sl]
        for j in range(HG):
            pr = slice(j * PD, (j + 1) * PD)
            tu_hi[pr, sl], tu_lo[pr, sl] = split(x_ref[j, :, sl].astype(F32) * tl[j:j + 1])
            sd_hi[pr, sl], sd_lo[pr, sl] = split(dy_ref[j, :, sl].astype(F32) * ec[j:j + 1])
    s_ref[...] = dot(tu_hi[...], b_ref[...]) + dot(tu_lo[...], b_ref[...])
    g_ref[...] = dot(sd_hi[...], c_ref[...]) + dot(sd_lo[...], c_ref[...])

    @pl.when(g == pl.num_programs(0) - 1)
    def _():
        wait_all(nd, me, got, send, recv)
        all_ref[...] = got[...]


def summaries(nd, x, dy, dt, par, b, c):
    t = x.shape[2]
    full = lambda shape: pl.BlockSpec(shape, lambda g: (0,) * len(shape))
    heads = pl.BlockSpec((HG, PD, t), lambda g: (g, 0, 0))
    state = pl.BlockSpec((HG * PD, N), lambda g: (g, 0))
    half = pltpu.VMEM((HG * PD, t), BF16)
    return pl.pallas_call(
        functools.partial(summary_kernel, nd),
        grid=(H // HG,),
        in_specs=[heads, heads, full((H, t)), full((H, L)), full((t, N)), full((t, N))],
        out_specs=[state, state, full((H, t)), full((H, L)), full((nd, 8, L))],
        out_shape=[jax.ShapeDtypeStruct((H * PD, N), F32), jax.ShapeDtypeStruct((H * PD, N), F32),
                   jax.ShapeDtypeStruct((H, t), F32), jax.ShapeDtypeStruct((H, L), F32), jax.ShapeDtypeStruct((nd, 8, L), F32)],
        scratch_shapes=[half, half, half, half, pltpu.VMEM((H, t), F32), pltpu.VMEM((H, t + L), F32), pltpu.VMEM((nd, 8, L), F32),
                        pltpu.SemaphoreType.DMA((nd,)), pltpu.SemaphoreType.DMA((nd,))],
        compiler_params=pltpu.CompilerParams(dimension_semantics=("arbitrary",), collective_id=1, has_side_effects=True),
        cost_estimate=pl.CostEstimate(flops=4 * H * PD * N * t * 2, bytes_accessed=4 * H * PD * t, transcendentals=0),
        name="range_summaries",
    )(x, dy, dt, par, b, c)


def tile_sum_kernel(nd, dh_ref, out_ref, got, send, recv):
    me = lax.axis_index(AXIS)
    got[me] = jnp.transpose(jnp.concatenate([dh_ref[...], jnp.zeros((L - H, L), F32)], axis=0))[:8]
    greet_all(nd, me)
    send_all(nd, me, got, send, recv)
    wait_all(nd, me, got, send, recv)
    total = got[0]
    for d in range(1, nd):
        total = total + got[d]
    out_ref[...] = total


def tile_sum(nd, dh):
    vm = pl.BlockSpec(memory_space=pltpu.VMEM)
    return pl.pallas_call(
        functools.partial(tile_sum_kernel, nd),
        in_specs=[vm], out_specs=vm, out_shape=jax.ShapeDtypeStruct((8, L), F32),
        scratch_shapes=[pltpu.VMEM((nd, 8, L), F32), pltpu.SemaphoreType.DMA((nd,)), pltpu.SemaphoreType.DMA((nd,))],
        compiler_params=pltpu.CompilerParams(collective_id=2, has_side_effects=True),
        name="tile_sum",
    )(dh)


CH = 2
KC = H // CH
HOP = 3


def chain_kernel(nd, tot_ref, s_ref, g_ref, s0_ref, g0_ref, so_ref, go_ref, s_out, g_out, s_send, s_recv, g_send, g_recv):
    me = lax.axis_index(AXIS)
    right, left = lax.rem(me + 1, nd), lax.rem(me + nd - 1, nd)
    barrier = pltpu.get_barrier_semaphore()
    for other in (left, right):
        pl.semaphore_signal(barrier, inc=1, device_id=(other,), device_id_type=pl.DeviceIdType.MESH)
    pl.semaphore_wait(barrier, 2)
    rows_of = lambda k: pl.ds(pl.multiple_of(k * CH * PD, CH * PD), CH * PD)

    def copy(out, into, send, recv, k, to):
        return pltpu.make_async_remote_copy(src_ref=out.at[rows_of(k)], dst_ref=into.at[rows_of(k)], send_sem=send.at[k], recv_sem=recv.at[k],
                                            device_id=(to,), device_id_type=pl.DeviceIdType.MESH)

    def pass_on(k, edge, last, to, first_ref, own_ref, into, out, send, recv):
        rows = rows_of(k)

        @pl.when(edge)
        def _():
            into[rows] = first_ref[rows]

        @pl.when(jnp.logical_not(edge))
        def _():
            copy(out, into, send, recv, k, to).wait_recv()

        @pl.when(jnp.logical_not(last))
        def _():
            for i in range(CH):
                r = pl.ds(pl.multiple_of(k * CH * PD + i * PD, PD), PD)
                decay = jnp.exp2(tot_ref[pl.ds(k * CH + i, 1), :])
                out[r] = decay * into[r] + own_ref[r]
            copy(out, into, send, recv, k, to).start()

    def step(n, _):
        ks, kg = n - HOP * me, n - HOP * (nd - 1 - me)

        @pl.when((ks >= 0) & (ks < KC))
        def _():
            pass_on(ks, me == 0, me == nd - 1, right, s0_ref, s_ref, so_ref, s_out, s_send, s_recv)

        @pl.when((kg >= 0) & (kg < KC))
        def _():
            pass_on(kg, me == nd - 1, me == 0, left, g0_ref, g_ref, go_ref, g_out, g_send, g_recv)
        return 0

    lax.fori_loop(0, HOP * (nd - 1) + KC, step, 0)

    def drain(k, _):
        @pl.when(me < nd - 1)
        def _():
            copy(s_out, so_ref, s_send, s_recv, k, right).wait_send()

        @pl.when(me > 0)
        def _():
            copy(g_out, go_ref, g_send, g_recv, k, left).wait_send()
        return 0

    lax.fori_loop(0, KC, drain, 0)


def chain(nd, tot, s_loc, g_loc, s0, g0):
    vm = pl.BlockSpec(memory_space=pltpu.VMEM)
    state = jax.ShapeDtypeStruct((H * PD, N), F32)
    return pl.pallas_call(
        functools.partial(chain_kernel, nd),
        in_specs=[vm] * 5,
        out_specs=[vm] * 2,
        out_shape=[state, state],
        scratch_shapes=[pltpu.VMEM((H * PD, N), F32), pltpu.VMEM((H * PD, N), F32)] + [pltpu.SemaphoreType.DMA((KC,))] * 4,
        compiler_params=pltpu.CompilerParams(collective_id=0, has_side_effects=True),
        cost_estimate=pl.CostEstimate(flops=10 ** 10, bytes_accessed=10 ** 7, transcendentals=0),
        name="state_chain",
    )(tot, s_loc, g_loc, s0, g0)


def local_kernel(x_ref, dy_ref, dt_ref, cs_ref, s0_ref, g1_ref, b_ref, c_ref, par_ref, dta_ref, para_ref,
                 dx_ref, ddt_ref, db_ref, dc_ref, dh_ref,
                 sf, gc, tu, sd, gh, us, gram, dg_acc, db_acc, dc_acc, ec_s, td_s, tl_s, ddir_s, xd_s, dcs_s, kd_s,
                 bb_ref, cc_ref, b2t_ref, ct_ref):
    nb = x_ref.shape[2] // L
    g = pl.program_id(0)
    below = lax.broadcasted_iota(jnp.int32, (L, L), 0) >= lax.broadcasted_iota(jnp.int32, (L, L), 1)
    lane = lax.broadcasted_iota(jnp.int32, (L, L), 1)

    @pl.when(g == 0)
    def _():
        for b in range(nb):
            bb, cc = b_ref[b * L:(b + 1) * L, :], c_ref[b * L:(b + 1) * L, :]
            gram[b] = dot(cc, bb, NT)
            bb_ref[b] = jnp.concatenate([bb, bb], axis=0)
            cc_ref[b] = jnp.concatenate([cc, cc], axis=0)
            bt = jnp.transpose(bb.astype(F32)).astype(BF16)
            b2t_ref[b] = jnp.concatenate([bt, bt], axis=0)
            ct_ref[b] = jnp.transpose(cc.astype(F32))
        dg_acc[...] = jnp.zeros_like(dg_acc)
        db_acc[...] = jnp.zeros_like(db_acc)
        dc_acc[...] = jnp.zeros_like(dc_acc)

    heads = pl.ds(pl.multiple_of(g * HG, HG), HG)
    for b in range(nb):
        sl = slice(b * L, (b + 1) * L)
        cs = cs_ref[:, sl]
        tail = jnp.exp2(cs[:, L - 1:L] - cs)
        ec_s[b] = jnp.exp2(cs)
        tl_s[b] = tail
        td_s[b] = tail * dt_ref[:, sl]

    sf[0] = s0_ref[...]

    def forward(b, _):
        toks = pl.ds(pl.multiple_of(b * L, L), L)
        etot = ec_s[b][:, L - 1:L]
        td = td_s[b]
        for j in range(HG):
            hi, lo = split(x_ref[j, :, toks].astype(F32) * td[j:j + 1])
            tu[b, j * PD:(j + 1) * PD, :L] = hi
            tu[b, j * PD:(j + 1) * PD, L:] = lo
        new = dot(tu[b], bb_ref[b])
        for j in range(HG):
            pr = slice(j * PD, (j + 1) * PD)
            sf[b + 1, pr] = etot[j:j + 1] * sf[b, pr] + new[pr]
        return 0

    lax.fori_loop(0, nb, forward, 0)
    gc[...] = g1_ref[...]

    def backward(i, _):
        b = nb - 1 - i
        toks = pl.ds(pl.multiple_of(b * L, L), L)
        ec, tl, cs, dtb = ec_s[b], tl_s[b], cs_ref[:, toks], dt_ref[:, toks]
        etot = ec[:, L - 1:L]
        cst = jnp.transpose(cs)
        kd = []
        for j in range(HG):
            pr = slice(j * PD, (j + 1) * PD)
            gj = gc[pr]
            kd.append(jnp.sum(gj * sf[b + 1, pr], axis=0, keepdims=True))
            hi, lo = split(gj)
            gh[pr, :L] = hi
            gh[pr, L:] = lo
            hi, lo = split(dy_ref[j, :, toks].astype(F32) * ec[j:j + 1])
            sd[pr, :L] = hi
            sd[pr, L:] = lo
        kd_s[b, heads] = jnp.concatenate(kd, axis=0)
        us[...] = dot(gh[...], b2t_ref[b])
        db_acc[b] += (dot(gh[:, :L], tu[b, :, :L], TN) + dot(gh[:, L:], tu[b, :, :L], TN)) + dot(gh[:, :L], tu[b, :, L:], TN)
        gram_b = gram[b]
        ct = ct_ref[b]
        dg = jnp.zeros((L, L), F32)
        dc = jnp.zeros((N, L), F32)
        rs_cols = jnp.zeros((L, L), F32)
        ddir, xd, inter = [], [], []
        for j in range(HG):
            pr = slice(j * PD, (j + 1) * PD)
            xj, dyj = x_ref[j, :, toks], dy_ref[j, :, toks]
            e = jnp.exp2(jnp.where(below, jnp.broadcast_to(cst[:, j:j + 1], (L, L)) - cs[j:j + 1], NEG))
            m = gram_b * e
            mhi, mlo = split(m)
            du = dot(jnp.concatenate([dyj, dyj], axis=1), jnp.concatenate([mhi, mlo], axis=0)) + us[pr] * tl[j:j + 1]
            dp = dot(dyj, xj, TN)
            w = dp * (e * dtb[j:j + 1])
            dg = dg + w
            rs = jnp.sum(w * gram_b, axis=1, keepdims=True)
            rs_cols = jnp.where(lane == j, jnp.broadcast_to(rs, (L, L)), rs_cols)
            xf, dyf = xj.astype(F32), dyj.astype(F32)
            ddir.append(jnp.sum(du * xf, axis=0, keepdims=True))
            xd.append(jnp.sum(dyf * xf, axis=0, keepdims=True))
            dx_ref[j, :, toks] = (du * dtb[j:j + 1] + dyf * par_ref[j:j + 1, 1:2]).astype(BF16)
            shi, slo = split(sf[b, pr])
            st = jnp.transpose(jnp.concatenate([shi, slo, shi, slo], axis=0))
            dhi, dlo = sd[pr, :L], sd[pr, L:]
            z = dot(st, jnp.concatenate([dhi, dhi, dlo, dlo], axis=0))
            dc = dc + z
            inter.append(jnp.sum(z * ct, axis=0, keepdims=True))
        dg_acc[b] += dg
        dc_acc[b] += dc
        ddir = jnp.concatenate(ddir, axis=0)
        ddir_s[b, heads] = ddir
        xd_s[b, heads] = jnp.concatenate(xd, axis=0)
        dcs_s[b, heads] = jnp.transpose(rs_cols)[:HG] + jnp.concatenate(inter, axis=0) - ddir * dtb
        grow = dot(sd[...], cc_ref[b])
        for j in range(HG):
            pr = slice(j * PD, (j + 1) * PD)
            gc[pr] = etot[j:j + 1] * gc[pr] + grow[pr]
        return 0

    lax.fori_loop(0, nb, backward, 0)

    @pl.when(g == pl.num_programs(0) - 1)
    def _():
        after = below.astype(F32)
        da_sum = jnp.zeros((H, 1), F32)
        dd_sum = jnp.zeros((H, 1), F32)
        for b in range(nb):
            sl = slice(b * L, (b + 1) * L)
            da = dot(dcs_s[b], after, precision=HIGHEST) + jnp.sum(kd_s[b], axis=1, keepdims=True)
            dta = da * para_ref[:, 0:1]
            ddt_ref[:, sl] = ddir_s[b] + dta
            da_sum += jnp.sum(dta * dta_ref[:, sl], axis=1, keepdims=True)
            dd_sum += jnp.sum(xd_s[b], axis=1, keepdims=True)
            ghi, glo = split(dg_acc[b])
            dbt = jnp.transpose(db_acc[b]) + (dot(ghi, cc_ref[b, :L, :], TN) + dot(glo, cc_ref[b, :L, :], TN))
            dct = jnp.transpose(dc_acc[b]) + (dot(ghi, bb_ref[b, :L, :]) + dot(glo, bb_ref[b, :L, :]))
            db_ref[sl, :] = dbt.astype(BF16)
            dc_ref[sl, :] = dct.astype(BF16)
        lane_h = lax.broadcasted_iota(jnp.int32, (H, L), 1)
        dh_ref[...] = jnp.where(lane_h == 0, da_sum, jnp.where(lane_h == 1, dd_sum, 0.0))


def local_backward(x, dy, dt, cs, s_start, ds_end, b, c, par):
    t = x.shape[2]
    nb = t // L
    full = lambda shape: pl.BlockSpec(shape, lambda g: (0,) * len(shape))
    heads = pl.BlockSpec((HG, PD, t), lambda g: (g, 0, 0))
    rows = pl.BlockSpec((HG, t), lambda g: (g, 0))
    state = pl.BlockSpec((HG * PD, N), lambda g: (g, 0))
    one = pl.BlockSpec((HG, L), lambda g: (g, 0))
    vm = lambda shape, dtype=F32: pltpu.VMEM(shape, dtype)
    return pl.pallas_call(
        local_kernel,
        grid=(H // HG,),
        in_specs=[heads, heads, rows, rows, state, state, full((t, N)), full((t, N)), one, full((H, t)), full((H, L))],
        out_specs=[heads, full((H, t)), full((t, N)), full((t, N)), full((H, L))],
        out_shape=[jax.ShapeDtypeStruct((H, PD, t), BF16), jax.ShapeDtypeStruct((H, t), F32), jax.ShapeDtypeStruct((t, N), BF16),
                   jax.ShapeDtypeStruct((t, N), BF16), jax.ShapeDtypeStruct((H, L), F32)],
        scratch_shapes=[vm((nb + 1, HG * PD, N)), vm((HG * PD, N)), vm((nb, HG * PD, 2 * L), BF16), vm((HG * PD, 2 * L), BF16),
                        vm((HG * PD, 2 * N), BF16), vm((HG * PD, L)), vm((nb, L, L)), vm((nb, L, L)), vm((nb, N, L)), vm((nb, N, L)),
                        vm((nb, HG, L)), vm((nb, HG, L)), vm((nb, HG, L)), vm((nb, H, L)), vm((nb, H, L)), vm((nb, H, L)), vm((nb, H, N)),
                        vm((nb, 2 * L, N), BF16), vm((nb, 2 * L, N), BF16), vm((nb, 2 * N, L), BF16), vm((nb, N, L))],
        compiler_params=pltpu.CompilerParams(dimension_semantics=("arbitrary",)),
        cost_estimate=pl.CostEstimate(flops=5 * 10 ** 10, bytes_accessed=6 * H * PD * t, transcendentals=H * t * L),
        name="local_backward",
    )(x, dy, dt, cs, s_start, ds_end, b, c, par, dt, par)


def solution(mesh):
    nd = mesh.shape[AXIS]
    tok4 = P(None, AXIS, None, None)
    tok3 = P(None, AXIS, None)

    def device_step(x_loc, dt_loc, a_log, b_loc, c_loc, d_skip, s_init, dy_loc, ds_last):
        x, dy = jnp.transpose(x_loc[0], (1, 2, 0)), jnp.transpose(dy_loc[0], (1, 2, 0))
        dt = jnp.transpose(dt_loc[0])
        b, c = b_loc[0], c_loc[0]
        col = jnp.arange(L)[None, :]
        par = jnp.where(col == 0, -jnp.exp(a_log)[:, None], jnp.where(col == 1, d_skip[:, None], 0.0))
        s_loc, g_loc, cs, tot, tot_all = summaries(nd, x, dy, dt, par, b, c)
        s0, g0 = s_init.reshape(H * PD, N), ds_last.reshape(H * PD, N)

        tot_all = tot_all[:, 0, :H]
        before = jnp.sum(jnp.where(jnp.arange(nd)[:, None] < lax.axis_index(AXIS), tot_all, 0.0), axis=0)
        part = jnp.exp2(before)[:, None, None] * g_loc.reshape(H, PD, N)
        ds_first = jnp.exp2(jnp.sum(tot_all, axis=0))[:, None, None] * ds_last[0] + lax.psum(part, AXIS)

        s_start, ds_end = chain(nd, tot, s_loc, g_loc, s0, g0)
        dx, ddt, db, dc, dh = local_backward(x, dy, dt, cs, s_start, ds_end, b, c, par)
        dh = tile_sum(nd, dh)
        return (jnp.transpose(dx, (2, 0, 1))[None], jnp.transpose(ddt)[None], db[None], dc[None], ds_first[None], dh[0, :H], dh[1, :H])

    return jax.shard_map(device_step, mesh=mesh,
                         in_specs=(tok4, tok3, P(), tok3, tok3, P(), P(), tok4, P()),
                         out_specs=(tok4, tok3, tok3, tok3, P(), P(), P()),
                         check_vma=False)
```

```python
import functools
import jax
import jax.numpy as jnp
from jax import lax
from jax.experimental import pallas as pl
from jax.experimental.pallas import tpu as pltpu
from jax.sharding import PartitionSpec as P

AXIS = 'cp'
H, PD, N = 80, 64, 128
L = 128
HG = 8
LOG2E = 1.4426950408889634
NEG = -1e30
F32, BF16 = jnp.float32, jnp.bfloat16
HIGHEST = lax.Precision.HIGHEST
NT = (((1,), (1,)), ((), ()))
TN = (((0,), (0,)), ((), ()))
NN = (((1,), (0,)), ((), ()))


def dot(a, b, dims=NN, precision=None):
    return lax.dot_general(a, b, dims, precision=precision, preferred_element_type=F32)


def split(v):
    hi = v.astype(BF16)
    return hi, (v - hi.astype(F32)).astype(BF16)


MESH = pl.DeviceIdType.MESH


def greet_all(nd, me):
    barrier = pltpu.get_barrier_semaphore()
    for o in range(1, nd):
        pl.semaphore_signal(barrier, inc=1, device_id=(lax.rem(me + o, nd),), device_id_type=MESH)
    pl.semaphore_wait(barrier, nd - 1)


def tile_copy(nd, me, o, got, send, recv):
    return pltpu.make_async_remote_copy(src_ref=got.at[me], dst_ref=got.at[me], send_sem=send.at[o], recv_sem=recv.at[o],
                                        device_id=(lax.rem(me + o, nd),), device_id_type=MESH)


def send_all(nd, me, got, send, recv):
    for o in range(1, nd):
        tile_copy(nd, me, o, got, send, recv).start()


def wait_all(nd, me, got, send, recv):
    for o in range(1, nd):
        src = lax.rem(me + nd - o, nd)
        pltpu.make_async_remote_copy(src_ref=got.at[src], dst_ref=got.at[src], send_sem=send.at[o], recv_sem=recv.at[o],
                                     device_id=(src,), device_id_type=MESH).wait_recv()
        tile_copy(nd, me, o, got, send, recv).wait_send()


def summary_kernel(x_ref, dy_ref, dt_ref, par_ref, b_ref, c_ref, s_ref, g_ref, cs_ref, tot_ref,
                   tu_hi, tu_lo, sd_hi, sd_lo, cs_all, off_all):
    nb = x_ref.shape[2] // L
    g = pl.program_id(0)

    @pl.when(g == 0)
    def _():
        tri = (lax.broadcasted_iota(jnp.int32, (L, L), 0) <= lax.broadcasted_iota(jnp.int32, (L, L), 1)).astype(F32)
        off = jnp.zeros((H, L), F32)
        for b in range(nb):
            sl = slice(b * L, (b + 1) * L)
            a = dt_ref[:, sl] * (par_ref[:, 0:1] * LOG2E)
            cs = dot(a, tri, precision=HIGHEST)
            cs_all[:, sl] = cs
            off_all[:, sl] = off
            off = off + jnp.broadcast_to(cs[:, L - 1:L], (H, L))
        off_all[:, nb * L:] = off
        cs_ref[...] = cs_all[...]
        tot_ref[...] = off

    rows = pl.ds(pl.multiple_of(g * HG, HG), HG)
    for b in range(nb):
        sl = slice(b * L, (b + 1) * L)
        run = cs_all[rows, sl] + off_all[rows, sl]
        ec = jnp.exp2(run)
        tl = jnp.exp2(off_all[rows, nb * L:] - run) * dt_ref[rows, sl]
        for j in range(HG):
            pr = slice(j * PD, (j + 1) * PD)
            tu_hi[pr, sl], tu_lo[pr, sl] = split(x_ref[j, :, sl].astype(F32) * tl[j:j + 1])
            sd_hi[pr, sl], sd_lo[pr, sl] = split(dy_ref[j, :, sl].astype(F32) * ec[j:j + 1])
    s_ref[...] = dot(tu_hi[...], b_ref[...]) + dot(tu_lo[...], b_ref[...])
    g_ref[...] = dot(sd_hi[...], c_ref[...]) + dot(sd_lo[...], c_ref[...])


def summaries(x, dy, dt, par, b, c):
    t = x.shape[2]
    full = lambda shape: pl.BlockSpec(shape, lambda g: (0,) * len(shape))
    heads = pl.BlockSpec((HG, PD, t), lambda g: (g, 0, 0))
    state = pl.BlockSpec((HG * PD, N), lambda g: (g, 0))
    half = pltpu.VMEM((HG * PD, t), BF16)
    return pl.pallas_call(
        summary_kernel,
        grid=(H // HG,),
        in_specs=[heads, heads, full((H, t)), full((H, L)), full((t, N)), full((t, N))],
        out_specs=[state, state, full((H, t)), full((H, L))],
        out_shape=[jax.ShapeDtypeStruct((H * PD, N), F32), jax.ShapeDtypeStruct((H * PD, N), F32),
                   jax.ShapeDtypeStruct((H, t), F32), jax.ShapeDtypeStruct((H, L), F32)],
        scratch_shapes=[half, half, half, half, pltpu.VMEM((H, t), F32), pltpu.VMEM((H, t + L), F32)],
        compiler_params=pltpu.CompilerParams(dimension_semantics=("arbitrary",)),
        cost_estimate=pl.CostEstimate(flops=4 * H * PD * N * t * 2, bytes_accessed=4 * H * PD * t, transcendentals=0),
        name="range_summaries",
    )(x, dy, dt, par, b, c)


def tile_sum_kernel(nd, dh_ref, out_ref, got, send, recv):
    me = lax.axis_index(AXIS)
    got[me] = jnp.transpose(jnp.concatenate([dh_ref[...], jnp.zeros((L - H, L), F32)], axis=0))[:8]
    greet_all(nd, me)
    send_all(nd, me, got, send, recv)
    wait_all(nd, me, got, send, recv)
    total = got[0]
    for d in range(1, nd):
        total = total + got[d]
    out_ref[...] = total


def tile_sum(nd, dh):
    vm = pl.BlockSpec(memory_space=pltpu.VMEM)
    return pl.pallas_call(
        functools.partial(tile_sum_kernel, nd),
        in_specs=[vm], out_specs=vm, out_shape=jax.ShapeDtypeStruct((8, L), F32),
        scratch_shapes=[pltpu.VMEM((nd, 8, L), F32), pltpu.SemaphoreType.DMA((nd,)), pltpu.SemaphoreType.DMA((nd,))],
        compiler_params=pltpu.CompilerParams(collective_id=2, has_side_effects=True),
        name="tile_sum",
    )(dh)


CH = 2
CR = CH * PD
KC = H // CH
CORE_HOP, CHIP_HOP = 2, 4
SLOTS = 2


def owner_of(nd, k):
    return jnp.where(k < nd, k, 4 * (k - nd) + 1)


def second_of(nd, me):
    return nd + (me - 1) // 4


def rows_of(k):
    return pl.ds(pl.multiple_of(k * CR, CR), CR)


def chain_kernel(nd, x_ref, dy_ref, dt_ref, cs_ref, b_ref, c_ref, tot_ref, s_ref, g_ref, s0_ref, g0_ref,
                 dui_ref, rs_ref, dg_ref, s_end, g_end, f_end,
                 gram, so_ref, go_ref, f_ref, s_out, g_out, f_out, first_sem, out_sem, s_send, s_recv, g_send, g_recv, f_send, f_recv):
    nb = x_ref.shape[2] // L
    g = pl.program_id(0)
    me = lax.axis_index(AXIS)
    last = nd - 1
    right, left = lax.rem(me + 1, nd), lax.rem(me + nd - 1, nd)

    def copy(out, into, send, recv, k, to):
        return pltpu.make_async_remote_copy(src_ref=out.at[rows_of(k)], dst_ref=into.at[rows_of(k)], send_sem=send.at[k], recv_sem=recv.at[k],
                                            device_id=(to,), device_id_type=MESH)

    def f_copy(k, slot, to):
        return pltpu.make_async_remote_copy(src_ref=f_out.at[rows_of(k)], dst_ref=f_ref.at[slot], send_sem=f_send.at[k], recv_sem=f_recv.at[slot],
                                            device_id=(to,), device_id_type=MESH)

    def combine(k, into, own_ref, out):
        for i in range(CH):
            r = pl.ds(pl.multiple_of(k * CR + i * PD, PD), PD)
            out[r] = jnp.exp2(tot_ref[pl.ds(k * CH + i, 1), :]) * into[r] + own_ref[r]

    def slot(n):
        rm = last - me
        ks = n - ((me // 2) * (CORE_HOP + CHIP_HOP) + (me % 2) * CORE_HOP)
        kg = n - ((rm // 2) * (CORE_HOP + CHIP_HOP) + (rm % 2) * CORE_HOP)

        @pl.when((ks >= 0) & (ks < KC))
        def _():
            @pl.when(me > 0)
            def _():
                copy(s_out, so_ref, s_send, s_recv, ks, right).wait_recv()

            @pl.when(me < last)
            def _():
                combine(ks, so_ref, s_ref, s_out)
                copy(s_out, so_ref, s_send, s_recv, ks, right).start()

        @pl.when((kg >= 0) & (kg < KC))
        def _():
            @pl.when(me < last)
            def _():
                copy(g_out, go_ref, g_send, g_recv, kg, left).wait_recv()

            @pl.when(me > 0)
            def _():
                combine(kg, go_ref, g_ref, g_out)
                copy(g_out, go_ref, g_send, g_recv, kg, left).start()

            @pl.when(me == 0)
            def _():
                combine(kg, go_ref, g_ref, f_out)

                @pl.when(kg == 0)
                def _():
                    f_ref[0] = f_out[rows_of(0)]

                @pl.when((kg > 0) & (kg < nd))
                def _():
                    f_copy(kg, 0, kg).start()

                @pl.when(kg >= nd)
                def _():
                    f_copy(kg, 1, 4 * (kg - nd) + 1).start()

    @pl.when(g == 0)
    def _():
        for b in range(nb):
            sl = slice(b * L, (b + 1) * L)
            gram[b] = dot(c_ref[sl, :], b_ref[sl, :], NT)
        dg_ref[...] = jnp.zeros_like(dg_ref)

        @pl.when(me == 0)
        def _():
            first = pltpu.make_async_copy(s0_ref, so_ref, first_sem)
            first.start()
            first.wait()

        @pl.when(me == last)
        def _():
            first = pltpu.make_async_copy(g0_ref, go_ref, first_sem)
            first.start()
            first.wait()

        greet_all(nd, me)

    below = lax.broadcasted_iota(jnp.int32, (L, L), 0) >= lax.broadcasted_iota(jnp.int32, (L, L), 1)
    lane = lax.broadcasted_iota(jnp.int32, (L, L), 1)

    def work(b, _):
        for p in range(SLOTS):
            slot((g * nb + b) * SLOTS + p)
        toks = pl.ds(pl.multiple_of(b * L, L), L)
        cs, dtb = cs_ref[:, toks], dt_ref[:, toks]
        cst = jnp.transpose(cs)
        gram_b = gram[b]
        dg = jnp.zeros((L, L), F32)
        rs_cols = jnp.zeros((L, L), F32)
        for j in range(HG):
            xj, dyj = x_ref[j, :, toks], dy_ref[j, :, toks]
            e = jnp.exp2(jnp.where(below, jnp.broadcast_to(cst[:, j:j + 1], (L, L)) - cs[j:j + 1], NEG))
            mhi, mlo = split(gram_b * e)
            dui_ref[j, :, toks] = dot(jnp.concatenate([dyj, dyj], axis=1), jnp.concatenate([mhi, mlo], axis=0))
            w = dot(dyj, xj, TN) * (e * dtb[j:j + 1])
            dg = dg + w
            rs = jnp.sum(w * gram_b, axis=1, keepdims=True)
            rs_cols = jnp.where(lane == j, jnp.broadcast_to(rs, (L, L)), rs_cols)
        dg_ref[b] += dg
        rs_ref[:, toks] = jnp.transpose(rs_cols)[:HG]
        return 0

    lax.fori_loop(0, nb, work, 0)

    @pl.when(g == pl.num_programs(0) - 1)
    def _():
        total = (last // 2) * (CORE_HOP + CHIP_HOP) + (last % 2) * CORE_HOP + KC

        def rest(n, _):
            slot(n)
            return 0

        lax.fori_loop((H // HG) * nb * SLOTS, total, rest, 0)

        outs = [pltpu.make_async_copy(so_ref, s_end, out_sem.at[0]), pltpu.make_async_copy(go_ref, g_end, out_sem.at[1])]
        for out in outs:
            out.start()

        def drain(k, _):
            @pl.when(me < last)
            def _():
                copy(s_out, so_ref, s_send, s_recv, k, right).wait_send()

            @pl.when(me > 0)
            def _():
                copy(g_out, go_ref, g_send, g_recv, k, left).wait_send()

            @pl.when((me == 0) & (k > 0))
            def _():
                f_copy(k, 0, last).wait_send()
            return 0

        lax.fori_loop(0, KC, drain, 0)

        @pl.when(me > 0)
        def _():
            f_copy(0, 0, 0).wait_recv()

        @pl.when(me % 4 == 1)
        def _():
            f_copy(0, 1, 0).wait_recv()

        @pl.when(me % 4 != 1)
        def _():
            f_ref[1] = jnp.zeros((CR, N), F32)

        f_end[...] = f_ref[...]
        for out in outs:
            out.wait()


def chain_and_blocks(nd, x, dy, dt, cs, b, c, tot, s_loc, g_loc, s0, g0):
    t = x.shape[2]
    nb = t // L
    full = lambda shape: pl.BlockSpec(shape, lambda g: (0,) * len(shape))
    heads = pl.BlockSpec((HG, PD, t), lambda g: (g, 0, 0))
    rows = pl.BlockSpec((HG, t), lambda g: (g, 0))
    anywhere = pl.BlockSpec(memory_space=pl.ANY)
    big = pltpu.VMEM((H * PD, N), F32)
    state = jax.ShapeDtypeStruct((H * PD, N), F32)
    return pl.pallas_call(
        functools.partial(chain_kernel, nd),
        grid=(H // HG,),
        in_specs=[heads, heads, rows, rows, full((t, N)), full((t, N)), full((H, L)), full((H * PD, N)), full((H * PD, N)), anywhere, anywhere],
        out_specs=[heads, rows, full((nb, L, L)), anywhere, anywhere, full((2, CR, N))],
        out_shape=[jax.ShapeDtypeStruct((H, PD, t), F32), jax.ShapeDtypeStruct((H, t), F32), jax.ShapeDtypeStruct((nb, L, L), F32), state, state,
                   jax.ShapeDtypeStruct((2, CR, N), F32)],
        scratch_shapes=[pltpu.VMEM((nb, L, L), F32), big, big, pltpu.VMEM((2, CR, N), F32), big, big, big, pltpu.SemaphoreType.DMA,
                        pltpu.SemaphoreType.DMA((2,))] + [pltpu.SemaphoreType.DMA((KC,))] * 5
                       + [pltpu.SemaphoreType.DMA((2,))],
        compiler_params=pltpu.CompilerParams(dimension_semantics=("arbitrary",), collective_id=0, has_side_effects=True),
        cost_estimate=pl.CostEstimate(flops=10 ** 10, bytes_accessed=10 ** 7, transcendentals=0),
        name="chain_and_blocks",
    )(x, dy, dt, cs, b, c, tot, s_loc, g_loc, s0, g0)


def carried_kernel(nd, x_ref, dy_ref, dt_ref, cs_ref, dui_ref, rs_ref, s0_ref, g1_ref, b_ref, c_ref, par_ref, dta_ref, para_ref, dg_ref, f_ref,
                   dx_ref, ddt_ref, db_ref, dc_ref, dh_ref, first_ref,
                   sf, gc, tu, sd, gh, us, db_acc, dc_acc, ec_s, td_s, tl_s, ddir_s, xd_s, dcs_s, kd_s, bb_ref, cc_ref, b2t_ref, ct_ref,
                   own_sem, f_send, f_recv):
    nb = x_ref.shape[2] // L
    g = pl.program_id(0)
    me = lax.axis_index(AXIS)
    barrier = pltpu.get_barrier_semaphore()
    has_second = me % 4 == 1

    def give(k, slot, o):
        return pltpu.make_async_remote_copy(src_ref=f_ref.at[slot], dst_ref=first_ref.at[rows_of(k)], send_sem=f_send.at[slot, o], recv_sem=f_recv.at[k],
                                            device_id=(lax.rem(me + o, nd),), device_id_type=MESH)

    def keep(k, slot):
        return pltpu.make_async_copy(f_ref.at[slot], first_ref.at[rows_of(k)], own_sem.at[slot])

    @pl.when(g == 0)
    def _():
        for o in range(1, nd):
            pl.semaphore_signal(barrier, inc=1, device_id=(lax.rem(me + o, nd),), device_id_type=MESH)
        for b in range(nb):
            bb, cc = b_ref[b * L:(b + 1) * L, :], c_ref[b * L:(b + 1) * L, :]
            bb_ref[b] = jnp.concatenate([bb, bb], axis=0)
            cc_ref[b] = jnp.concatenate([cc, cc], axis=0)
            bt = jnp.transpose(bb.astype(F32)).astype(BF16)
            b2t_ref[b] = jnp.concatenate([bt, bt], axis=0)
            ct_ref[b] = jnp.transpose(cc.astype(F32))
        db_acc[...] = jnp.zeros_like(db_acc)
        dc_acc[...] = jnp.zeros_like(dc_acc)

    @pl.when(g == 1)
    def _():
        pl.semaphore_wait(barrier, nd - 1)
        keep(me, 0).start()
        for o in range(1, nd):
            give(me, 0, o).start()

        @pl.when(has_second)
        def _():
            keep(second_of(nd, me), 1).start()
            for o in range(1, nd):
                give(second_of(nd, me), 1, o).start()

    heads = pl.ds(pl.multiple_of(g * HG, HG), HG)
    for b in range(nb):
        sl = slice(b * L, (b + 1) * L)
        cs = cs_ref[:, sl]
        tail = jnp.exp2(cs[:, L - 1:L] - cs)
        ec_s[b] = jnp.exp2(cs)
        tl_s[b] = tail
        td_s[b] = tail * dt_ref[:, sl]

    sf[0] = s0_ref[...]

    def forward(b, _):
        toks = pl.ds(pl.multiple_of(b * L, L), L)
        etot = ec_s[b][:, L - 1:L]
        td = td_s[b]
        for j in range(HG):
            hi, lo = split(x_ref[j, :, toks].astype(F32) * td[j:j + 1])
            tu[b, j * PD:(j + 1) * PD, :L] = hi
            tu[b, j * PD:(j + 1) * PD, L:] = lo
        new = dot(tu[b], bb_ref[b])
        for j in range(HG):
            pr = slice(j * PD, (j + 1) * PD)
            sf[b + 1, pr] = etot[j:j + 1] * sf[b, pr] + new[pr]
        return 0

    lax.fori_loop(0, nb, forward, 0)
    gc[...] = g1_ref[...]

    def backward(i, _):
        b = nb - 1 - i
        toks = pl.ds(pl.multiple_of(b * L, L), L)
        ec, tl, dtb = ec_s[b], tl_s[b], dt_ref[:, toks]
        etot = ec[:, L - 1:L]
        kd = []
        for j in range(HG):
            pr = slice(j * PD, (j + 1) * PD)
            gj = gc[pr]
            kd.append(jnp.sum(gj * sf[b + 1, pr], axis=0, keepdims=True))
            hi, lo = split(gj)
            gh[pr, :L] = hi
            gh[pr, L:] = lo
            hi, lo = split(dy_ref[j, :, toks].astype(F32) * ec[j:j + 1])
            sd[pr, :L] = hi
            sd[pr, L:] = lo
        kd_s[b, heads] = jnp.concatenate(kd, axis=0)
        us[...] = dot(gh[...], b2t_ref[b])
        db_acc[b] += (dot(gh[:, :L], tu[b, :, :L], TN) + dot(gh[:, L:], tu[b, :, :L], TN)) + dot(gh[:, :L], tu[b, :, L:], TN)
        ct = ct_ref[b]
        dc = jnp.zeros((N, L), F32)
        ddir, xd, inter = [], [], []
        for j in range(HG):
            pr = slice(j * PD, (j + 1) * PD)
            du = dui_ref[j, :, toks] + us[pr] * tl[j:j + 1]
            xf, dyf = x_ref[j, :, toks].astype(F32), dy_ref[j, :, toks].astype(F32)
            ddir.append(jnp.sum(du * xf, axis=0, keepdims=True))
            xd.append(jnp.sum(dyf * xf, axis=0, keepdims=True))
            dx_ref[j, :, toks] = (du * dtb[j:j + 1] + dyf * par_ref[j:j + 1, 1:2]).astype(BF16)
            shi, slo = split(sf[b, pr])
            st = jnp.transpose(jnp.concatenate([shi, slo, shi, slo], axis=0))
            dhi, dlo = sd[pr, :L], sd[pr, L:]
            z = dot(st, jnp.concatenate([dhi, dhi, dlo, dlo], axis=0))
            dc = dc + z
            inter.append(jnp.sum(z * ct, axis=0, keepdims=True))
        dc_acc[b] += dc
        ddir = jnp.concatenate(ddir, axis=0)
        ddir_s[b, heads] = ddir
        xd_s[b, heads] = jnp.concatenate(xd, axis=0)
        dcs_s[b, heads] = rs_ref[:, toks] + jnp.concatenate(inter, axis=0) - ddir * dtb
        grow = dot(sd[...], cc_ref[b])
        for j in range(HG):
            pr = slice(j * PD, (j + 1) * PD)
            gc[pr] = etot[j:j + 1] * gc[pr] + grow[pr]
        return 0

    lax.fori_loop(0, nb, backward, 0)

    @pl.when(g == pl.num_programs(0) - 1)
    def _():
        after = (lax.broadcasted_iota(jnp.int32, (L, L), 0) >= lax.broadcasted_iota(jnp.int32, (L, L), 1)).astype(F32)
        da_sum = jnp.zeros((H, 1), F32)
        dd_sum = jnp.zeros((H, 1), F32)
        for b in range(nb):
            sl = slice(b * L, (b + 1) * L)
            da = dot(dcs_s[b], after, precision=HIGHEST) + jnp.sum(kd_s[b], axis=1, keepdims=True)
            dta = da * para_ref[:, 0:1]
            ddt_ref[:, sl] = ddir_s[b] + dta
            da_sum += jnp.sum(dta * dta_ref[:, sl], axis=1, keepdims=True)
            dd_sum += jnp.sum(xd_s[b], axis=1, keepdims=True)
            ghi, glo = split(dg_ref[b])
            dbt = jnp.transpose(db_acc[b]) + (dot(ghi, cc_ref[b, :L, :], TN) + dot(glo, cc_ref[b, :L, :], TN))
            dct = jnp.transpose(dc_acc[b]) + (dot(ghi, bb_ref[b, :L, :]) + dot(glo, bb_ref[b, :L, :]))
            db_ref[sl, :] = dbt.astype(BF16)
            dc_ref[sl, :] = dct.astype(BF16)
        lane_h = lax.broadcasted_iota(jnp.int32, (H, L), 1)
        dh_ref[...] = jnp.where(lane_h == 0, da_sum, jnp.where(lane_h == 1, dd_sum, 0.0))
        keep(me, 0).wait()
        for o in range(1, nd):
            give(me, 0, o).wait_send()

        @pl.when(has_second)
        def _():
            keep(second_of(nd, me), 1).wait()
            for o in range(1, nd):
                give(second_of(nd, me), 1, o).wait_send()

        for k in range(KC):
            @pl.when(me != (k if k < nd else 4 * (k - nd) + 1))
            def _():
                give(k, 0, 1).wait_recv()


def carried(nd, x, dy, dt, cs, dui, rs, s_start, ds_end, b, c, par, dg, f):
    t = x.shape[2]
    nb = t // L
    full = lambda shape: pl.BlockSpec(shape, lambda g: (0,) * len(shape))
    heads = pl.BlockSpec((HG, PD, t), lambda g: (g, 0, 0))
    rows = pl.BlockSpec((HG, t), lambda g: (g, 0))
    state = pl.BlockSpec((HG * PD, N), lambda g: (g, 0))
    one = pl.BlockSpec((HG, L), lambda g: (g, 0))
    vm = lambda shape, dtype=F32: pltpu.VMEM(shape, dtype)
    return pl.pallas_call(
        functools.partial(carried_kernel, nd),
        grid=(H // HG,),
        in_specs=[heads, heads, rows, rows, heads, rows, state, state, full((t, N)), full((t, N)), one, full((H, t)), full((H, L)),
                  full((nb, L, L)), full((2, CR, N))],
        out_specs=[heads, full((H, t)), full((t, N)), full((t, N)), full((H, L)), pl.BlockSpec(memory_space=pl.ANY)],
        out_shape=[jax.ShapeDtypeStruct((H, PD, t), BF16), jax.ShapeDtypeStruct((H, t), F32), jax.ShapeDtypeStruct((t, N), BF16),
                   jax.ShapeDtypeStruct((t, N), BF16), jax.ShapeDtypeStruct((H, L), F32), jax.ShapeDtypeStruct((H * PD, N), F32)],
        scratch_shapes=[vm((nb + 1, HG * PD, N)), vm((HG * PD, N)), vm((nb, HG * PD, 2 * L), BF16), vm((HG * PD, 2 * L), BF16),
                        vm((HG * PD, 2 * N), BF16), vm((HG * PD, L)), vm((nb, N, L)), vm((nb, N, L)),
                        vm((nb, HG, L)), vm((nb, HG, L)), vm((nb, HG, L)), vm((nb, H, L)), vm((nb, H, L)), vm((nb, H, L)), vm((nb, H, N)),
                        vm((nb, 2 * L, N), BF16), vm((nb, 2 * L, N), BF16), vm((nb, 2 * N, L), BF16), vm((nb, N, L)),
                        pltpu.SemaphoreType.DMA((2,)), pltpu.SemaphoreType.DMA((2, nd)), pltpu.SemaphoreType.DMA((KC,))],
        compiler_params=pltpu.CompilerParams(dimension_semantics=("arbitrary",), collective_id=1, has_side_effects=True),
        cost_estimate=pl.CostEstimate(flops=5 * 10 ** 10, bytes_accessed=6 * H * PD * t, transcendentals=H * t * L),
        name="carried_backward",
    )(x, dy, dt, cs, dui, rs, s_start, ds_end, b, c, par, dt, par, dg, f)


def solution(mesh):
    nd = mesh.shape[AXIS]
    tok4 = P(None, AXIS, None, None)
    tok3 = P(None, AXIS, None)

    def device_step(x_loc, dt_loc, a_log, b_loc, c_loc, d_skip, s_init, dy_loc, ds_last):
        x, dy = jnp.transpose(x_loc[0], (1, 2, 0)), jnp.transpose(dy_loc[0], (1, 2, 0))
        dt = jnp.transpose(dt_loc[0])
        b, c = b_loc[0], c_loc[0]
        col = jnp.arange(L)[None, :]
        par = jnp.where(col == 0, -jnp.exp(a_log)[:, None], jnp.where(col == 1, d_skip[:, None], 0.0))
        s_loc, g_loc, cs, tot = summaries(x, dy, dt, par, b, c)
        s0, g0 = s_init.reshape(H * PD, N), ds_last.reshape(H * PD, N)
        dui, rs, dg, s_start, ds_end, f = chain_and_blocks(nd, x, dy, dt, cs, b, c, tot, s_loc, g_loc, s0, g0)
        dx, ddt, db, dc, dh, first = carried(nd, x, dy, dt, cs, dui, rs, s_start, ds_end, b, c, par, dg, f)
        dh = tile_sum(nd, dh)
        return (jnp.transpose(dx, (2, 0, 1))[None], jnp.transpose(ddt)[None], db[None], dc[None], first.reshape(1, H, PD, N), dh[0, :H], dh[1, :H])

    return jax.shard_map(device_step, mesh=mesh,
                         in_specs=(tok4, tok3, P(), tok3, tok3, P(), P(), tok4, P()),
                         out_specs=(tok4, tok3, tok3, tok3, P(), P(), P()),
                         check_vma=False)
```

```python
import functools
import jax
import jax.numpy as jnp
from jax import lax
from jax.experimental import pallas as pl
from jax.experimental.pallas import tpu as pltpu
from jax.sharding import PartitionSpec as P

AXIS = 'cp'
H, PD, N = 80, 64, 128
L = 128
HG = 8
LOG2E = 1.4426950408889634
NEG = -1e30
F32, BF16 = jnp.float32, jnp.bfloat16
HIGHEST = lax.Precision.HIGHEST
NT = (((1,), (1,)), ((), ()))
TN = (((0,), (0,)), ((), ()))
NN = (((1,), (0,)), ((), ()))


def dot(a, b, dims=NN, precision=None):
    return lax.dot_general(a, b, dims, precision=precision, preferred_element_type=F32)


def split(v):
    hi = v.astype(BF16)
    return hi, (v - hi.astype(F32)).astype(BF16)


MESH = pl.DeviceIdType.MESH


def greet_all(nd, me):
    barrier = pltpu.get_barrier_semaphore()
    for o in range(1, nd):
        pl.semaphore_signal(barrier, inc=1, device_id=(lax.rem(me + o, nd),), device_id_type=MESH)
    pl.semaphore_wait(barrier, nd - 1)


def tile_copy(nd, me, o, got, send, recv):
    return pltpu.make_async_remote_copy(src_ref=got.at[me], dst_ref=got.at[me], send_sem=send.at[o], recv_sem=recv.at[o],
                                        device_id=(lax.rem(me + o, nd),), device_id_type=MESH)


def send_all(nd, me, got, send, recv):
    for o in range(1, nd):
        tile_copy(nd, me, o, got, send, recv).start()


def wait_all(nd, me, got, send, recv):
    for o in range(1, nd):
        src = lax.rem(me + nd - o, nd)
        pltpu.make_async_remote_copy(src_ref=got.at[src], dst_ref=got.at[src], send_sem=send.at[o], recv_sem=recv.at[o],
                                     device_id=(src,), device_id_type=MESH).wait_recv()
        tile_copy(nd, me, o, got, send, recv).wait_send()


def summary_kernel(x_ref, dy_ref, dt_ref, par_ref, b_ref, c_ref, s_ref, g_ref, cs_ref, tot_ref,
                   tu_hi, tu_lo, sd_hi, sd_lo, cs_all, off_all):
    nb = x_ref.shape[2] // L
    g = pl.program_id(0)

    @pl.when(g == 0)
    def _():
        tri = (lax.broadcasted_iota(jnp.int32, (L, L), 0) <= lax.broadcasted_iota(jnp.int32, (L, L), 1)).astype(F32)
        off = jnp.zeros((H, L), F32)
        for b in range(nb):
            sl = slice(b * L, (b + 1) * L)
            a = dt_ref[:, sl] * (par_ref[:, 0:1] * LOG2E)
            cs = dot(a, tri, precision=HIGHEST)
            cs_all[:, sl] = cs
            off_all[:, sl] = off
            off = off + jnp.broadcast_to(cs[:, L - 1:L], (H, L))
        off_all[:, nb * L:] = off
        cs_ref[...] = cs_all[...]
        tot_ref[...] = off

    rows = pl.ds(pl.multiple_of(g * HG, HG), HG)
    for b in range(nb):
        sl = slice(b * L, (b + 1) * L)
        run = cs_all[rows, sl] + off_all[rows, sl]
        ec = jnp.exp2(run)
        tl = jnp.exp2(off_all[rows, nb * L:] - run) * dt_ref[rows, sl]
        for j in range(HG):
            pr = slice(j * PD, (j + 1) * PD)
            tu_hi[pr, sl], tu_lo[pr, sl] = split(x_ref[j, :, sl].astype(F32) * tl[j:j + 1])
            sd_hi[pr, sl], sd_lo[pr, sl] = split(dy_ref[j, :, sl].astype(F32) * ec[j:j + 1])
    s_ref[...] = dot(tu_hi[...], b_ref[...]) + dot(tu_lo[...], b_ref[...])
    g_ref[...] = dot(sd_hi[...], c_ref[...]) + dot(sd_lo[...], c_ref[...])


def summaries(x, dy, dt, par, b, c):
    t = x.shape[2]
    full = lambda shape: pl.BlockSpec(shape, lambda g: (0,) * len(shape))
    heads = pl.BlockSpec((HG, PD, t), lambda g: (g, 0, 0))
    state = pl.BlockSpec((HG * PD, N), lambda g: (g, 0))
    half = pltpu.VMEM((HG * PD, t), BF16)
    return pl.pallas_call(
        summary_kernel,
        grid=(H // HG,),
        in_specs=[heads, heads, full((H, t)), full((H, L)), full((t, N)), full((t, N))],
        out_specs=[state, state, full((H, t)), full((H, L))],
        out_shape=[jax.ShapeDtypeStruct((H * PD, N), F32), jax.ShapeDtypeStruct((H * PD, N), F32),
                   jax.ShapeDtypeStruct((H, t), F32), jax.ShapeDtypeStruct((H, L), F32)],
        scratch_shapes=[half, half, half, half, pltpu.VMEM((H, t), F32), pltpu.VMEM((H, t + L), F32)],
        compiler_params=pltpu.CompilerParams(dimension_semantics=("arbitrary",)),
        cost_estimate=pl.CostEstimate(flops=4 * H * PD * N * t * 2, bytes_accessed=4 * H * PD * t, transcendentals=0),
        name="range_summaries",
    )(x, dy, dt, par, b, c)


def tile_sum_kernel(nd, dh_ref, out_ref, got, send, recv):
    me = lax.axis_index(AXIS)
    got[me] = jnp.transpose(jnp.concatenate([dh_ref[...], jnp.zeros((L - H, L), F32)], axis=0))[:8]
    greet_all(nd, me)
    send_all(nd, me, got, send, recv)
    wait_all(nd, me, got, send, recv)
    total = got[0]
    for d in range(1, nd):
        total = total + got[d]
    out_ref[...] = total


def tile_sum(nd, dh):
    vm = pl.BlockSpec(memory_space=pltpu.VMEM)
    return pl.pallas_call(
        functools.partial(tile_sum_kernel, nd),
        in_specs=[vm], out_specs=vm, out_shape=jax.ShapeDtypeStruct((8, L), F32),
        scratch_shapes=[pltpu.VMEM((nd, 8, L), F32), pltpu.SemaphoreType.DMA((nd,)), pltpu.SemaphoreType.DMA((nd,))],
        compiler_params=pltpu.CompilerParams(collective_id=2, has_side_effects=True),
        name="tile_sum",
    )(dh)


GD = 4
QH = H // GD
QR = QH * PD
HOP = 3
BACK = 3


def chain_kernel(nd, x_ref, dy_ref, dt_ref, cs_ref, b_ref, c_ref, tot_ref, s_hbm, g_hbm, s0_ref, g0_ref,
                 dui_ref, rs_ref, dg_ref, s_end, g_end, f_ref,
                 gram, tots, own, par, tq, tx, xin, cin, cout, bsend, brecv, dsend, into, local_sem, tot_send, tot_recv, par_send, par_recv,
                 x_send, x_recv, c_send, c_recv, b_send, b_recv, d_send, d_recv, out_sem):
    nb = x_ref.shape[2] // L
    ng = nd // GD
    g = pl.program_id(0)
    me = lax.axis_index(AXIS)
    q, core, chip, pos = lax.rem(me, 4), lax.rem(me, 2), lax.rem(me // 2, 2), me // 4
    other_core, other_chip = me + 1 - 2 * core, me + 2 - 4 * chip
    oq = lax.rem(q + 2, 4)
    local = (s_hbm, g_hbm)

    def rows(head, n=1):
        return pl.ds(pl.multiple_of(head * PD, PD), n * PD)

    def remote(src, dst, send, recv, to):
        return pltpu.make_async_remote_copy(src_ref=src, dst_ref=dst, send_sem=send, recv_sem=recv, device_id=(to,), device_id_type=MESH)

    def tot_copy(o):
        return remote(tot_ref, tots.at[q], tot_send.at[o], tot_recv.at[o], 4 * pos + lax.rem(q + o, 4))

    def tot_got(o):
        src = lax.rem(q + 4 - o, 4)
        return remote(tot_ref, tots.at[src], tot_send.at[o], tot_recv.at[o], 4 * pos + src)

    def par_copy(d, i):
        return remote(local[d].at[rows(QH * (2 * i + 1 - core), QH)], par.at[d, i], par_send.at[d, i], par_recv.at[d, i], other_core)

    def x_copy(d, k):
        return remote(tx.at[d, rows(k)], xin.at[d, rows(k)], x_send.at[d, k], x_recv.at[d, k], other_chip)

    def c_copy(d, k):
        return remote(cout.at[d, rows(k)], cin.at[d, rows(k)], c_send.at[d, k], c_recv.at[d, k], me + (4 - 8 * d))

    def b_copy(d, k):
        return remote(bsend.at[d, rows(k)], brecv.at[d, rows(k)], b_send.at[d, k], b_recv.at[d, k], other_chip)

    def d_copy(d, i, k):
        head = QH * (2 * i + core) + k
        return remote(dsend.at[d, i, rows(k)], into.at[d, rows(head)], d_send.at[d, i, k], d_recv.at[d, i, k], other_core)

    def decay(qq, head):
        return tots[qq, pl.ds(head, 1), :]

    def core_level(d, i, k, state):
        head = QH * (2 * i + core) + k
        mine_near = core == d
        near = jnp.where(mine_near, own[d, rows(head)], par[d, i, rows(k)])
        e_near = jnp.exp2(decay(2 * chip + d, head))
        far = e_near * state + near
        into[d, rows(head)] = jnp.where(mine_near, state, far)
        dsend[d, i, rows(k)] = jnp.where(mine_near, far, state)
        d_copy(d, i, k).start()

    def chain_step(d, k):
        head = QH * q + k
        has_prev = (pos > 0) if d == 0 else (pos < ng - 1)
        has_next = (pos < ng - 1) if d == 0 else (pos > 0)
        x_copy(d, k).wait_recv()

        @pl.when(has_prev)
        def _():
            c_copy(d, k).wait_recv()

        mine_near = chip == d
        state = cin[d, rows(k)]
        near = jnp.where(mine_near, tq[d, rows(k)], xin[d, rows(k)])
        afar = jnp.where(mine_near, xin[d, rows(k)], tq[d, rows(k)])
        e_near = jnp.exp2(decay(2 * d, head) + decay(2 * d + 1, head))
        e_far = jnp.exp2(decay(2 - 2 * d, head) + decay(3 - 2 * d, head))
        far = e_near * state + near
        cout[d, rows(k)] = e_far * far + afar

        @pl.when(has_next)
        def _():
            c_copy(d, k).start()

        bsend[d, rows(k)] = jnp.where(mine_near, far, state)
        b_copy(d, k).start()
        core_level(d, chip, k, jnp.where(mine_near, state, far))

    def back_step(d, k):
        b_copy(d, k).wait_recv()
        core_level(d, 1 - chip, k, brecv[d, rows(k)])

    def slot(n):
        for d in range(2):
            k = n - HOP * (pos if d == 0 else ng - 1 - pos)

            @pl.when((k >= 0) & (k < QH))
            def _():
                chain_step(d, k)

            @pl.when((k >= BACK) & (k < QH + BACK))
            def _():
                back_step(d, k - BACK)

    @pl.when(g == 0)
    def _():
        locals_ = [pltpu.make_async_copy(s_hbm, own.at[0], local_sem.at[0]), pltpu.make_async_copy(g_hbm, own.at[1], local_sem.at[1]),
                   pltpu.make_async_copy(tot_ref, tots.at[q], local_sem.at[2]),
                   pltpu.make_async_copy(s0_ref.at[rows(QH * q, QH)], cin.at[0], local_sem.at[3]),
                   pltpu.make_async_copy(g0_ref.at[rows(QH * q, QH)], cin.at[1], local_sem.at[4])]
        for cp in locals_[:3]:
            cp.start()

        @pl.when(pos == 0)
        def _():
            locals_[3].start()
            locals_[3].wait()

        @pl.when(pos == ng - 1)
        def _():
            locals_[4].start()
            locals_[4].wait()

        greet_all(nd, me)
        for o in range(1, GD):
            tot_copy(o).start()
        for d in range(2):
            for i in range(2):
                par_copy(d, i).start()
        for b in range(nb):
            sl = slice(b * L, (b + 1) * L)
            gram[b] = dot(c_ref[sl, :], b_ref[sl, :], NT)
        dg_ref[...] = jnp.zeros_like(dg_ref)
        for cp in locals_[:3]:
            cp.wait()
        for o in range(1, GD):
            tot_got(o).wait_recv()
        for d in range(2):
            for i in range(2):
                par_copy(d, i).wait_recv()

        def combine(d, i, k):
            head = QH * (2 * i + core) + k
            mine_near = core == d
            mine, his = own[d, rows(head)], par[d, i, rows(k)]
            e_far = jnp.exp2(decay(2 * chip + 1 - d, head))
            return e_far * jnp.where(mine_near, mine, his) + jnp.where(mine_near, his, mine)

        def front(k, _):
            for d in range(2):
                tx[d, rows(k)] = combine(d, 1 - chip, k)
                x_copy(d, k).start()
                tq[d, rows(k)] = combine(d, chip, k)
            return 0

        lax.fori_loop(0, QH, front, 0)

    below = lax.broadcasted_iota(jnp.int32, (L, L), 0) >= lax.broadcasted_iota(jnp.int32, (L, L), 1)
    lane = lax.broadcasted_iota(jnp.int32, (L, L), 1)

    def work(b, _):
        slot(g * nb + b)
        toks = pl.ds(pl.multiple_of(b * L, L), L)
        cs, dtb = cs_ref[:, toks], dt_ref[:, toks]
        cst = jnp.transpose(cs)
        gram_b = gram[b]
        dg = jnp.zeros((L, L), F32)
        rs_cols = jnp.zeros((L, L), F32)
        for j in range(HG):
            xj, dyj = x_ref[j, :, toks], dy_ref[j, :, toks]
            e = jnp.exp2(jnp.where(below, jnp.broadcast_to(cst[:, j:j + 1], (L, L)) - cs[j:j + 1], NEG))
            mhi, mlo = split(gram_b * e)
            dui_ref[j, :, toks] = dot(jnp.concatenate([dyj, dyj], axis=1), jnp.concatenate([mhi, mlo], axis=0))
            w = dot(dyj, xj, TN) * (e * dtb[j:j + 1])
            dg = dg + w
            rs = jnp.sum(w * gram_b, axis=1, keepdims=True)
            rs_cols = jnp.where(lane == j, jnp.broadcast_to(rs, (L, L)), rs_cols)
        dg_ref[b] += dg
        rs_ref[:, toks] = jnp.transpose(rs_cols)[:HG]
        return 0

    lax.fori_loop(0, nb, work, 0)

    @pl.when(g == pl.num_programs(0) - 1)
    def _():
        def rest(n, _):
            slot(n)
            return 0

        lax.fori_loop((H // HG) * nb, HOP * (ng - 1) + QH + BACK, rest, 0)

        def drain(k, _):
            for d in range(2):
                x_copy(d, k).wait_send()
                b_copy(d, k).wait_send()

                @pl.when((pos < ng - 1) if d == 0 else (pos > 0))
                def _():
                    c_copy(d, k).wait_send()

                for i in range(2):
                    d_copy(d, i, k).wait()
            return 0

        lax.fori_loop(0, QH, drain, 0)
        outs = [pltpu.make_async_copy(into.at[0], s_end, out_sem.at[0]), pltpu.make_async_copy(into.at[1], g_end, out_sem.at[1])]
        for out in outs:
            out.start()
        for o in range(1, GD):
            tot_copy(o).wait_send()
        for d in range(2):
            for i in range(2):
                par_copy(d, i).wait_send()
        f_ref[...] = cout[1]
        for out in outs:
            out.wait()


def chain_and_blocks(nd, x, dy, dt, cs, b, c, tot, s_loc, g_loc, s0, g0):
    t = x.shape[2]
    nb = t // L
    full = lambda shape: pl.BlockSpec(shape, lambda g: (0,) * len(shape))
    heads = pl.BlockSpec((HG, PD, t), lambda g: (g, 0, 0))
    rows = pl.BlockSpec((HG, t), lambda g: (g, 0))
    anywhere = pl.BlockSpec(memory_space=pl.ANY)
    quarter = pltpu.VMEM((2, QR, N), F32)
    whole = pltpu.VMEM((2, H * PD, N), F32)
    halves = pltpu.VMEM((2, 2, QR, N), F32)
    sems = lambda *shape: pltpu.SemaphoreType.DMA(shape)
    state = jax.ShapeDtypeStruct((H * PD, N), F32)
    return pl.pallas_call(
        functools.partial(chain_kernel, nd),
        grid=(H // HG,),
        in_specs=[heads, heads, rows, rows, full((t, N)), full((t, N))] + [anywhere] * 5,
        out_specs=[heads, rows, full((nb, L, L)), anywhere, anywhere, full((QR, N))],
        out_shape=[jax.ShapeDtypeStruct((H, PD, t), F32), jax.ShapeDtypeStruct((H, t), F32), jax.ShapeDtypeStruct((nb, L, L), F32), state, state,
                   jax.ShapeDtypeStruct((QR, N), F32)],
        scratch_shapes=[pltpu.VMEM((nb, L, L), F32), pltpu.VMEM((GD, H, L), F32), whole, halves] + [quarter] * 7 + [halves, whole]
                       + [sems(5), sems(GD), sems(GD), sems(2, 2), sems(2, 2)] + [sems(2, QH)] * 6 + [sems(2, 2, QH)] * 2 + [sems(2)],
        compiler_params=pltpu.CompilerParams(dimension_semantics=("arbitrary",), collective_id=0, has_side_effects=True),
        cost_estimate=pl.CostEstimate(flops=10 ** 10, bytes_accessed=10 ** 7, transcendentals=0),
        name="chain_and_blocks",
    )(x, dy, dt, cs, b, c, tot, s_loc, g_loc, s0, g0)


FC = 5
FR = QR // FC
F_HOP = 5


def carried_kernel(nd, x_ref, dy_ref, dt_ref, cs_ref, dui_ref, rs_ref, s0_ref, g1_ref, b_ref, c_ref, par_ref, dta_ref, para_ref, dg_ref, f_ref,
                   dx_ref, ddt_ref, db_ref, dc_ref, dh_ref, first_ref,
                   sf, gc, tu, sd, gh, us, db_acc, dc_acc, ec_s, td_s, tl_s, ddir_s, xd_s, dcs_s, kd_s, bb_ref, cc_ref, b2t_ref, ct_ref,
                   fq, own_sem, f_send, f_recv, p_send, p_recv):
    nb = x_ref.shape[2] // L
    g = pl.program_id(0)
    me = lax.axis_index(AXIS)
    barrier = pltpu.get_barrier_semaphore()
    ng = nd // GD
    q, pos = lax.rem(me, 4), me // 4

    def part(k):
        return pl.ds(pl.multiple_of(k * FR, FR), FR)

    def remote(src, dst, send, recv, to):
        return pltpu.make_async_remote_copy(src_ref=src, dst_ref=dst, send_sem=send, recv_sem=recv, device_id=(to,), device_id_type=MESH)

    def f_copy(k):
        return remote(fq.at[part(k)], fq.at[part(k)], f_send.at[k], f_recv.at[k], me + 4)

    def give(o, k):
        return remote(fq.at[part(k)], first_ref.at[part(q * FC + k)], p_send.at[o, k], p_recv.at[o, k], 4 * pos + lax.rem(q + o, 4))

    def given(o, k):
        src = lax.rem(q + 4 - o, 4)
        return remote(fq.at[part(k)], first_ref.at[part(src * FC + k)], p_send.at[o, k], p_recv.at[o, k], 4 * pos + src)

    def keep(k):
        return pltpu.make_async_copy(fq.at[part(k)], first_ref.at[part(q * FC + k)], own_sem.at[k])

    def first_step(k):
        @pl.when(pos > 0)
        def _():
            f_copy(k).wait_recv()

        @pl.when(pos < ng - 1)
        def _():
            f_copy(k).start()

        keep(k).start()
        for o in range(1, GD):
            give(o, k).start()

    @pl.when(g == 0)
    def _():
        for o in range(1, nd):
            pl.semaphore_signal(barrier, inc=1, device_id=(lax.rem(me + o, nd),), device_id_type=MESH)
        for b in range(nb):
            bb, cc = b_ref[b * L:(b + 1) * L, :], c_ref[b * L:(b + 1) * L, :]
            bb_ref[b] = jnp.concatenate([bb, bb], axis=0)
            cc_ref[b] = jnp.concatenate([cc, cc], axis=0)
            bt = jnp.transpose(bb.astype(F32)).astype(BF16)
            b2t_ref[b] = jnp.concatenate([bt, bt], axis=0)
            ct_ref[b] = jnp.transpose(cc.astype(F32))
        db_acc[...] = jnp.zeros_like(db_acc)
        dc_acc[...] = jnp.zeros_like(dc_acc)

    @pl.when(g == 1)
    def _():
        pl.semaphore_wait(barrier, nd - 1)

        @pl.when(pos == 0)
        def _():
            fq[...] = f_ref[...]

    heads = pl.ds(pl.multiple_of(g * HG, HG), HG)
    for b in range(nb):
        sl = slice(b * L, (b + 1) * L)
        cs = cs_ref[:, sl]
        tail = jnp.exp2(cs[:, L - 1:L] - cs)
        ec_s[b] = jnp.exp2(cs)
        tl_s[b] = tail
        td_s[b] = tail * dt_ref[:, sl]

    sf[0] = s0_ref[...]

    def forward(b, _):
        toks = pl.ds(pl.multiple_of(b * L, L), L)
        etot = ec_s[b][:, L - 1:L]
        td = td_s[b]
        for j in range(HG):
            hi, lo = split(x_ref[j, :, toks].astype(F32) * td[j:j + 1])
            tu[b, j * PD:(j + 1) * PD, :L] = hi
            tu[b, j * PD:(j + 1) * PD, L:] = lo
        new = dot(tu[b], bb_ref[b])
        for j in range(HG):
            pr = slice(j * PD, (j + 1) * PD)
            sf[b + 1, pr] = etot[j:j + 1] * sf[b, pr] + new[pr]
        return 0

    lax.fori_loop(0, nb, forward, 0)
    gc[...] = g1_ref[...]

    def backward(i, _):
        b = nb - 1 - i
        k = (g - 1) * nb + i - F_HOP * pos

        @pl.when((k >= 0) & (k < FC))
        def _():
            first_step(k)

        toks = pl.ds(pl.multiple_of(b * L, L), L)
        ec, tl, dtb = ec_s[b], tl_s[b], dt_ref[:, toks]
        etot = ec[:, L - 1:L]
        kd = []
        for j in range(HG):
            pr = slice(j * PD, (j + 1) * PD)
            gj = gc[pr]
            kd.append(jnp.sum(gj * sf[b + 1, pr], axis=0, keepdims=True))
            hi, lo = split(gj)
            gh[pr, :L] = hi
            gh[pr, L:] = lo
            hi, lo = split(dy_ref[j, :, toks].astype(F32) * ec[j:j + 1])
            sd[pr, :L] = hi
            sd[pr, L:] = lo
        kd_s[b, heads] = jnp.concatenate(kd, axis=0)
        us[...] = dot(gh[...], b2t_ref[b])
        db_acc[b] += (dot(gh[:, :L], tu[b, :, :L], TN) + dot(gh[:, L:], tu[b, :, :L], TN)) + dot(gh[:, :L], tu[b, :, L:], TN)
        ct = ct_ref[b]
        dc = jnp.zeros((N, L), F32)
        ddir, xd, inter = [], [], []
        for j in range(HG):
            pr = slice(j * PD, (j + 1) * PD)
            du = dui_ref[j, :, toks] + us[pr] * tl[j:j + 1]
            xf, dyf = x_ref[j, :, toks].astype(F32), dy_ref[j, :, toks].astype(F32)
            ddir.append(jnp.sum(du * xf, axis=0, keepdims=True))
            xd.append(jnp.sum(dyf * xf, axis=0, keepdims=True))
            dx_ref[j, :, toks] = (du * dtb[j:j + 1] + dyf * par_ref[j:j + 1, 1:2]).astype(BF16)
            shi, slo = split(sf[b, pr])
            st = jnp.transpose(jnp.concatenate([shi, slo, shi, slo], axis=0))
            dhi, dlo = sd[pr, :L], sd[pr, L:]
            z = dot(st, jnp.concatenate([dhi, dhi, dlo, dlo], axis=0))
            dc = dc + z
            inter.append(jnp.sum(z * ct, axis=0, keepdims=True))
        dc_acc[b] += dc
        ddir = jnp.concatenate(ddir, axis=0)
        ddir_s[b, heads] = ddir
        xd_s[b, heads] = jnp.concatenate(xd, axis=0)
        dcs_s[b, heads] = rs_ref[:, toks] + jnp.concatenate(inter, axis=0) - ddir * dtb
        grow = dot(sd[...], cc_ref[b])
        for j in range(HG):
            pr = slice(j * PD, (j + 1) * PD)
            gc[pr] = etot[j:j + 1] * gc[pr] + grow[pr]
        return 0

    lax.fori_loop(0, nb, backward, 0)

    @pl.when(g == pl.num_programs(0) - 1)
    def _():
        after = (lax.broadcasted_iota(jnp.int32, (L, L), 0) >= lax.broadcasted_iota(jnp.int32, (L, L), 1)).astype(F32)
        da_sum = jnp.zeros((H, 1), F32)
        dd_sum = jnp.zeros((H, 1), F32)
        for b in range(nb):
            sl = slice(b * L, (b + 1) * L)
            da = dot(dcs_s[b], after, precision=HIGHEST) + jnp.sum(kd_s[b], axis=1, keepdims=True)
            dta = da * para_ref[:, 0:1]
            ddt_ref[:, sl] = ddir_s[b] + dta
            da_sum += jnp.sum(dta * dta_ref[:, sl], axis=1, keepdims=True)
            dd_sum += jnp.sum(xd_s[b], axis=1, keepdims=True)
            ghi, glo = split(dg_ref[b])
            dbt = jnp.transpose(db_acc[b]) + (dot(ghi, cc_ref[b, :L, :], TN) + dot(glo, cc_ref[b, :L, :], TN))
            dct = jnp.transpose(dc_acc[b]) + (dot(ghi, bb_ref[b, :L, :]) + dot(glo, bb_ref[b, :L, :]))
            db_ref[sl, :] = dbt.astype(BF16)
            dc_ref[sl, :] = dct.astype(BF16)
        lane_h = lax.broadcasted_iota(jnp.int32, (H, L), 1)
        dh_ref[...] = jnp.where(lane_h == 0, da_sum, jnp.where(lane_h == 1, dd_sum, 0.0))
        for k in range(FC):
            keep(k).wait()

            @pl.when(pos < ng - 1)
            def _():
                f_copy(k).wait_send()

            for o in range(1, GD):
                give(o, k).wait_send()
                given(o, k).wait_recv()


def carried(nd, x, dy, dt, cs, dui, rs, s_start, ds_end, b, c, par, dg, f):
    t = x.shape[2]
    nb = t // L
    full = lambda shape: pl.BlockSpec(shape, lambda g: (0,) * len(shape))
    heads = pl.BlockSpec((HG, PD, t), lambda g: (g, 0, 0))
    rows = pl.BlockSpec((HG, t), lambda g: (g, 0))
    state = pl.BlockSpec((HG * PD, N), lambda g: (g, 0))
    one = pl.BlockSpec((HG, L), lambda g: (g, 0))
    vm = lambda shape, dtype=F32: pltpu.VMEM(shape, dtype)
    return pl.pallas_call(
        functools.partial(carried_kernel, nd),
        grid=(H // HG,),
        in_specs=[heads, heads, rows, rows, heads, rows, state, state, full((t, N)), full((t, N)), one, full((H, t)), full((H, L)),
                  full((nb, L, L)), full((QR, N))],
        out_specs=[heads, full((H, t)), full((t, N)), full((t, N)), full((H, L)), pl.BlockSpec(memory_space=pl.ANY)],
        out_shape=[jax.ShapeDtypeStruct((H, PD, t), BF16), jax.ShapeDtypeStruct((H, t), F32), jax.ShapeDtypeStruct((t, N), BF16),
                   jax.ShapeDtypeStruct((t, N), BF16), jax.ShapeDtypeStruct((H, L), F32), jax.ShapeDtypeStruct((H * PD, N), F32)],
        scratch_shapes=[vm((nb + 1, HG * PD, N)), vm((HG * PD, N)), vm((nb, HG * PD, 2 * L), BF16), vm((HG * PD, 2 * L), BF16),
                        vm((HG * PD, 2 * N), BF16), vm((HG * PD, L)), vm((nb, N, L)), vm((nb, N, L)),
                        vm((nb, HG, L)), vm((nb, HG, L)), vm((nb, HG, L)), vm((nb, H, L)), vm((nb, H, L)), vm((nb, H, L)), vm((nb, H, N)),
                        vm((nb, 2 * L, N), BF16), vm((nb, 2 * L, N), BF16), vm((nb, 2 * N, L), BF16), vm((nb, N, L)),
                        vm((QR, N))] + [pltpu.SemaphoreType.DMA((FC,))] * 3 + [pltpu.SemaphoreType.DMA((GD, FC))] * 2,
        compiler_params=pltpu.CompilerParams(dimension_semantics=("arbitrary",), collective_id=1, has_side_effects=True),
        cost_estimate=pl.CostEstimate(flops=5 * 10 ** 10, bytes_accessed=6 * H * PD * t, transcendentals=H * t * L),
        name="carried_backward",
    )(x, dy, dt, cs, dui, rs, s_start, ds_end, b, c, par, dt, par, dg, f)


def solution(mesh):
    nd = mesh.shape[AXIS]
    tok4 = P(None, AXIS, None, None)
    tok3 = P(None, AXIS, None)

    def device_step(x_loc, dt_loc, a_log, b_loc, c_loc, d_skip, s_init, dy_loc, ds_last):
        x, dy = jnp.transpose(x_loc[0], (1, 2, 0)), jnp.transpose(dy_loc[0], (1, 2, 0))
        dt = jnp.transpose(dt_loc[0])
        b, c = b_loc[0], c_loc[0]
        col = jnp.arange(L)[None, :]
        par = jnp.where(col == 0, -jnp.exp(a_log)[:, None], jnp.where(col == 1, d_skip[:, None], 0.0))
        s_loc, g_loc, cs, tot = summaries(x, dy, dt, par, b, c)
        s0, g0 = s_init.reshape(H * PD, N), ds_last.reshape(H * PD, N)
        dui, rs, dg, s_start, ds_end, f = chain_and_blocks(nd, x, dy, dt, cs, b, c, tot, s_loc, g_loc, s0, g0)
        dx, ddt, db, dc, dh, first = carried(nd, x, dy, dt, cs, dui, rs, s_start, ds_end, b, c, par, dg, f)
        dh = tile_sum(nd, dh)
        return (jnp.transpose(dx, (2, 0, 1))[None], jnp.transpose(ddt)[None], db[None], dc[None], first.reshape(1, H, PD, N), dh[0, :H], dh[1, :H])

    return jax.shard_map(device_step, mesh=mesh,
                         in_specs=(tok4, tok3, P(), tok3, tok3, P(), P(), tok4, P()),
                         out_specs=(tok4, tok3, tok3, tok3, P(), P(), P()),
                         check_vma=False)
```

```python
import functools
import jax
import jax.numpy as jnp
from jax import lax
from jax.experimental import pallas as pl
from jax.experimental.pallas import tpu as pltpu
from jax.sharding import PartitionSpec as P

AXIS = 'cp'
H, PD, N = 80, 64, 128
L = 128
HG = 8
LOG2E = 1.4426950408889634
NEG = -1e30
F32, BF16 = jnp.float32, jnp.bfloat16
HIGHEST = lax.Precision.HIGHEST
NT = (((1,), (1,)), ((), ()))
TN = (((0,), (0,)), ((), ()))
NN = (((1,), (0,)), ((), ()))


def dot(a, b, dims=NN, precision=None):
    return lax.dot_general(a, b, dims, precision=precision, preferred_element_type=F32)


def split(v):
    hi = v.astype(BF16)
    return hi, (v - hi.astype(F32)).astype(BF16)


MESH = pl.DeviceIdType.MESH


def greet_all(nd, me):
    barrier = pltpu.get_barrier_semaphore()
    for o in range(1, nd):
        pl.semaphore_signal(barrier, inc=1, device_id=(lax.rem(me + o, nd),), device_id_type=MESH)
    pl.semaphore_wait(barrier, nd - 1)


def tile_copy(nd, me, o, got, send, recv):
    return pltpu.make_async_remote_copy(src_ref=got.at[me], dst_ref=got.at[me], send_sem=send.at[o], recv_sem=recv.at[o],
                                        device_id=(lax.rem(me + o, nd),), device_id_type=MESH)


def send_all(nd, me, got, send, recv):
    for o in range(1, nd):
        tile_copy(nd, me, o, got, send, recv).start()


def wait_all(nd, me, got, send, recv):
    for o in range(1, nd):
        src = lax.rem(me + nd - o, nd)
        pltpu.make_async_remote_copy(src_ref=got.at[src], dst_ref=got.at[src], send_sem=send.at[o], recv_sem=recv.at[o],
                                     device_id=(src,), device_id_type=MESH).wait_recv()
        tile_copy(nd, me, o, got, send, recv).wait_send()


def summary_kernel(x_ref, dy_ref, dt_ref, par_ref, b_ref, c_ref, s_ref, g_ref, cs_ref, tot_ref,
                   tu_hi, tu_lo, sd_hi, sd_lo, cs_all, off_all):
    nb = x_ref.shape[2] // L
    g = pl.program_id(0)

    @pl.when(g == 0)
    def _():
        tri = (lax.broadcasted_iota(jnp.int32, (L, L), 0) <= lax.broadcasted_iota(jnp.int32, (L, L), 1)).astype(F32)
        off = jnp.zeros((H, L), F32)
        for b in range(nb):
            sl = slice(b * L, (b + 1) * L)
            a = dt_ref[:, sl] * (par_ref[:, 0:1] * LOG2E)
            cs = dot(a, tri, precision=HIGHEST)
            cs_all[:, sl] = cs
            off_all[:, sl] = off
            off = off + jnp.broadcast_to(cs[:, L - 1:L], (H, L))
        off_all[:, nb * L:] = off
        cs_ref[...] = cs_all[...]
        tot_ref[...] = off

    rows = pl.ds(pl.multiple_of(g * HG, HG), HG)
    for b in range(nb):
        sl = slice(b * L, (b + 1) * L)
        run = cs_all[rows, sl] + off_all[rows, sl]
        ec = jnp.exp2(run)
        tl = jnp.exp2(off_all[rows, nb * L:] - run) * dt_ref[rows, sl]
        for j in range(HG):
            pr = slice(j * PD, (j + 1) * PD)
            tu_hi[pr, sl], tu_lo[pr, sl] = split(x_ref[j, :, sl].astype(F32) * tl[j:j + 1])
            sd_hi[pr, sl], sd_lo[pr, sl] = split(dy_ref[j, :, sl].astype(F32) * ec[j:j + 1])
    s_ref[...] = dot(tu_hi[...], b_ref[...]) + dot(tu_lo[...], b_ref[...])
    g_ref[...] = dot(sd_hi[...], c_ref[...]) + dot(sd_lo[...], c_ref[...])


def summaries(x, dy, dt, par, b, c):
    t = x.shape[2]
    full = lambda shape: pl.BlockSpec(shape, lambda g: (0,) * len(shape))
    heads = pl.BlockSpec((HG, PD, t), lambda g: (g, 0, 0))
    state = pl.BlockSpec((HG * PD, N), lambda g: (g, 0))
    half = pltpu.VMEM((HG * PD, t), BF16)
    return pl.pallas_call(
        summary_kernel,
        grid=(H // HG,),
        in_specs=[heads, heads, full((H, t)), full((H, L)), full((t, N)), full((t, N))],
        out_specs=[state, state, full((H, t)), full((H, L))],
        out_shape=[jax.ShapeDtypeStruct((H * PD, N), F32), jax.ShapeDtypeStruct((H * PD, N), F32),
                   jax.ShapeDtypeStruct((H, t), F32), jax.ShapeDtypeStruct((H, L), F32)],
        scratch_shapes=[half, half, half, half, pltpu.VMEM((H, t), F32), pltpu.VMEM((H, t + L), F32)],
        compiler_params=pltpu.CompilerParams(dimension_semantics=("arbitrary",)),
        cost_estimate=pl.CostEstimate(flops=4 * H * PD * N * t * 2, bytes_accessed=4 * H * PD * t, transcendentals=0),
        name="range_summaries",
    )(x, dy, dt, par, b, c)


def tile_sum_kernel(nd, dh_ref, out_ref, got, send, recv):
    me = lax.axis_index(AXIS)
    got[me] = jnp.transpose(jnp.concatenate([dh_ref[...], jnp.zeros((L - H, L), F32)], axis=0))[:8]
    greet_all(nd, me)
    send_all(nd, me, got, send, recv)
    wait_all(nd, me, got, send, recv)
    total = got[0]
    for d in range(1, nd):
        total = total + got[d]
    out_ref[...] = total


def tile_sum(nd, dh):
    vm = pl.BlockSpec(memory_space=pltpu.VMEM)
    return pl.pallas_call(
        functools.partial(tile_sum_kernel, nd),
        in_specs=[vm], out_specs=vm, out_shape=jax.ShapeDtypeStruct((8, L), F32),
        scratch_shapes=[pltpu.VMEM((nd, 8, L), F32), pltpu.SemaphoreType.DMA((nd,)), pltpu.SemaphoreType.DMA((nd,))],
        compiler_params=pltpu.CompilerParams(collective_id=2, has_side_effects=True),
        name="tile_sum",
    )(dh)


GD = 4
QH = H // GD
QR = QH * PD
F_BACK = 4
HOP = 3
BACK = 18


def chain_kernel(nd, x_ref, dy_ref, dt_ref, cs_ref, b_ref, c_ref, tot_ref, s_hbm, g_hbm, s0_ref, g0_ref,
                 dui_ref, rs_ref, dg_ref, s_end, g_end, first_ref,
                 gram, tots, own, par, tq, tx, xin, cin, cout, bsend, brecv, dsend, into, rsum, pick, fq, fxr, local_sem, tot_send, tot_recv, par_send, par_recv,
                 x_send, x_recv, c_send, c_recv, b_send, b_recv, d_send, d_recv, f_send, f_recv, fx_send, fx_recv, fd_send, fd_recv, out_sem):
    nb = x_ref.shape[2] // L
    ng = nd // GD
    g = pl.program_id(0)
    me = lax.axis_index(AXIS)
    q, core, chip, pos = lax.rem(me, 4), lax.rem(me, 2), lax.rem(me // 2, 2), me // 4
    other_core, other_chip = me + 1 - 2 * core, me + 2 - 4 * chip
    oq = lax.rem(q + 2, 4)
    local = (s_hbm, g_hbm)

    def rows(head, n=1):
        return pl.ds(pl.multiple_of(head * PD, PD), n * PD)

    def remote(src, dst, send, recv, to):
        return pltpu.make_async_remote_copy(src_ref=src, dst_ref=dst, send_sem=send, recv_sem=recv, device_id=(to,), device_id_type=MESH)

    def tot_copy(o):
        return remote(tot_ref, tots.at[q], tot_send.at[o], tot_recv.at[o], 4 * pos + lax.rem(q + o, 4))

    def tot_got(o):
        src = lax.rem(q + 4 - o, 4)
        return remote(tot_ref, tots.at[src], tot_send.at[o], tot_recv.at[o], 4 * pos + src)

    def par_copy(d, i):
        return remote(local[d].at[rows(QH * (2 * i + 1 - core), QH)], par.at[d, i], par_send.at[d, i], par_recv.at[d, i], other_core)

    def x_copy(d, k):
        return remote(tx.at[d, rows(k)], xin.at[d, rows(k)], x_send.at[d, k], x_recv.at[d, k], other_chip)

    def c_copy(d, k):
        return remote(cout.at[d, rows(k)], cin.at[d, rows(k)], c_send.at[d, k], c_recv.at[d, k], me + (4 - 8 * d))

    def b_copy(d, k):
        return remote(bsend.at[d, rows(k)], brecv.at[d, rows(k)], b_send.at[d, k], b_recv.at[d, k], other_chip)

    def d_copy(d, i, k):
        head = QH * (2 * i + core) + k
        return remote(dsend.at[d, i, rows(k)], into.at[d, rows(head)], d_send.at[d, i, k], d_recv.at[d, i, k], other_core)

    def f_copy(k):
        return remote(fq.at[rows(k)], fq.at[rows(k)], f_send.at[k], f_recv.at[k], me + 4)

    def fx_copy(k):
        return remote(fq.at[rows(k)], fxr.at[rows(k)], fx_send.at[k], fx_recv.at[k], other_chip)

    def fd_copy(i, k):
        src, head = (fq, QH * q + k) if i == 0 else (fxr, QH * oq + k)
        return remote(src.at[rows(k)], first_ref.at[rows(head)], fd_send.at[i, k], fd_recv.at[i, k], other_core)

    def f_step(k):
        @pl.when(pos > 0)
        def _():
            f_copy(k).wait_recv()

        @pl.when(pos < ng - 1)
        def _():
            f_copy(k).start()

        fx_copy(k).start()
        fd_copy(0, k).start()

    def f_back(k):
        fx_copy(k).wait_recv()
        fd_copy(1, k).start()

    def decay(qq, head):
        return tots[qq, pl.ds(head, 1), :]

    def core_level(d, i, k, state):
        head = QH * (2 * i + core) + k
        mine_near = core == d
        near = jnp.where(mine_near, own[d, rows(head)], par[d, i, rows(k)])
        e_near = jnp.exp2(decay(2 * chip + d, head))
        far = e_near * state + near
        into[d, rows(head)] = jnp.where(mine_near, state, far)
        dsend[d, i, rows(k)] = jnp.where(mine_near, far, state)
        d_copy(d, i, k).start()

    def chain_step(d, k):
        head = QH * q + k
        has_prev = (pos > 0) if d == 0 else (pos < ng - 1)
        has_next = (pos < ng - 1) if d == 0 else (pos > 0)
        x_copy(d, k).wait_recv()

        @pl.when(has_prev)
        def _():
            c_copy(d, k).wait_recv()

        mine_near = chip == d
        state = cin[d, rows(k)]
        near = jnp.where(mine_near, tq[d, rows(k)], xin[d, rows(k)])
        afar = jnp.where(mine_near, xin[d, rows(k)], tq[d, rows(k)])
        e_near = jnp.exp2(decay(2 * d, head) + decay(2 * d + 1, head))
        e_far = jnp.exp2(decay(2 - 2 * d, head) + decay(3 - 2 * d, head))
        far = e_near * state + near
        out = e_far * far + afar
        cout[d, rows(k)] = out

        if d == 1:
            @pl.when(pos == 0)
            def _():
                fq[rows(k)] = out

        @pl.when(has_next)
        def _():
            c_copy(d, k).start()

        bsend[d, rows(k)] = jnp.where(mine_near, far, state)
        b_copy(d, k).start()
        core_level(d, chip, k, jnp.where(mine_near, state, far))

    def back_step(d, k):
        b_copy(d, k).wait_recv()
        core_level(d, 1 - chip, k, brecv[d, rows(k)])

    def slot(n):
        for d in range(2):
            k = n - HOP * (pos if d == 0 else ng - 1 - pos)

            @pl.when((k >= 0) & (k < QH))
            def _():
                chain_step(d, k)

            @pl.when((k >= BACK) & (k < QH + BACK))
            def _():
                back_step(d, k - BACK)

        kf = n - (HOP * (ng - 1 + pos) + 1)

        @pl.when((kf >= 0) & (kf < QH))
        def _():
            f_step(kf)

        @pl.when((kf >= F_BACK) & (kf < QH + F_BACK))
        def _():
            f_back(kf - F_BACK)

    @pl.when(g == 0)
    def _():
        locals_ = [pltpu.make_async_copy(s_hbm, own.at[0], local_sem.at[0]), pltpu.make_async_copy(g_hbm, own.at[1], local_sem.at[1]),
                   pltpu.make_async_copy(tot_ref, tots.at[q], local_sem.at[2]),
                   pltpu.make_async_copy(s0_ref.at[rows(QH * q, QH)], cin.at[0], local_sem.at[3]),
                   pltpu.make_async_copy(g0_ref.at[rows(QH * q, QH)], cin.at[1], local_sem.at[4])]
        for cp in locals_[:3]:
            cp.start()

        @pl.when(pos == 0)
        def _():
            locals_[3].start()
            locals_[3].wait()

        @pl.when(pos == ng - 1)
        def _():
            locals_[4].start()
            locals_[4].wait()

        greet_all(nd, me)
        for o in range(1, GD):
            tot_copy(o).start()
        for d in range(2):
            for i in range(2):
                par_copy(d, i).start()
        for b in range(nb):
            sl = slice(b * L, (b + 1) * L)
            gram[b] = dot(c_ref[sl, :], b_ref[sl, :], NT)
        dg_ref[...] = jnp.zeros_like(dg_ref)
        for j in range(2 * HG):
            pick[j * L:(j + 1) * L, :] = (lax.broadcasted_iota(jnp.int32, (L, L), 1) == j // 2).astype(F32).astype(BF16)
        for cp in locals_[:3]:
            cp.wait()
        for o in range(1, GD):
            tot_got(o).wait_recv()
        for d in range(2):
            for i in range(2):
                par_copy(d, i).wait_recv()

        def combine(d, i, k):
            head = QH * (2 * i + core) + k
            mine_near = core == d
            mine, his = own[d, rows(head)], par[d, i, rows(k)]
            e_far = jnp.exp2(decay(2 * chip + 1 - d, head))
            return e_far * jnp.where(mine_near, mine, his) + jnp.where(mine_near, his, mine)

        def front(k, _):
            for d in range(2):
                tx[d, rows(k)] = combine(d, 1 - chip, k)
                x_copy(d, k).start()
                tq[d, rows(k)] = combine(d, chip, k)
            return 0

        lax.fori_loop(0, QH, front, 0)

    below = lax.broadcasted_iota(jnp.int32, (L, L), 0) >= lax.broadcasted_iota(jnp.int32, (L, L), 1)

    def work(b, _):
        slot(g * nb + b)
        toks = pl.ds(pl.multiple_of(b * L, L), L)
        cs, dtb = cs_ref[:, toks], dt_ref[:, toks]
        cst = jnp.transpose(cs)
        gram_b = gram[b]
        dg = jnp.zeros((L, L), F32)
        for j in range(HG):
            xj, dyj = x_ref[j, :, toks], dy_ref[j, :, toks]
            e = jnp.exp2(jnp.where(below, jnp.broadcast_to(cst[:, j:j + 1], (L, L)) - cs[j:j + 1], NEG))
            mhi, mlo = split(gram_b * e)
            dui_ref[j, :, toks] = dot(jnp.concatenate([dyj, dyj], axis=1), jnp.concatenate([mhi, mlo], axis=0))
            w = dot(dyj, xj, TN) * (e * dtb[j:j + 1])
            dg = dg + w
            rsum[:, (2 * j) * L:(2 * j + 1) * L], rsum[:, (2 * j + 1) * L:(2 * j + 2) * L] = split(w * gram_b)
        dg_ref[b] += dg
        rs_ref[:, toks] = jnp.transpose(dot(rsum[...], pick[...]))[:HG]
        return 0

    lax.fori_loop(0, nb, work, 0)

    @pl.when(g == pl.num_programs(0) - 1)
    def _():
        def rest(n, _):
            slot(n)
            return 0

        lax.fori_loop((H // HG) * nb, 2 * HOP * (ng - 1) + 1 + QH + F_BACK, rest, 0)

        def drain(k, _):
            for d in range(2):
                x_copy(d, k).wait_send()
                b_copy(d, k).wait_send()

                @pl.when((pos < ng - 1) if d == 0 else (pos > 0))
                def _():
                    c_copy(d, k).wait_send()

                for i in range(2):
                    d_copy(d, i, k).wait()

            @pl.when(pos < ng - 1)
            def _():
                f_copy(k).wait_send()

            fx_copy(k).wait_send()
            for i in range(2):
                fd_copy(i, k).wait()
            return 0

        early = [pltpu.make_async_copy(fq, first_ref.at[rows(QH * q, QH)], out_sem.at[2]),
                 pltpu.make_async_copy(fxr, first_ref.at[rows(QH * oq, QH)], out_sem.at[3])]
        for out in early:
            out.start()
        lax.fori_loop(0, QH, drain, 0)
        outs = [pltpu.make_async_copy(into.at[0], s_end, out_sem.at[0]), pltpu.make_async_copy(into.at[1], g_end, out_sem.at[1])]
        for out in outs:
            out.start()
        for o in range(1, GD):
            tot_copy(o).wait_send()
        for d in range(2):
            for i in range(2):
                par_copy(d, i).wait_send()
        for out in early + outs:
            out.wait()


def chain_and_blocks(nd, x, dy, dt, cs, b, c, tot, s_loc, g_loc, s0, g0):
    t = x.shape[2]
    nb = t // L
    full = lambda shape: pl.BlockSpec(shape, lambda g: (0,) * len(shape))
    heads = pl.BlockSpec((HG, PD, t), lambda g: (g, 0, 0))
    rows = pl.BlockSpec((HG, t), lambda g: (g, 0))
    anywhere = pl.BlockSpec(memory_space=pl.ANY)
    quarter = pltpu.VMEM((2, QR, N), F32)
    whole = pltpu.VMEM((2, H * PD, N), F32)
    halves = pltpu.VMEM((2, 2, QR, N), F32)
    sems = lambda *shape: pltpu.SemaphoreType.DMA(shape)
    state = jax.ShapeDtypeStruct((H * PD, N), F32)
    return pl.pallas_call(
        functools.partial(chain_kernel, nd),
        grid=(H // HG,),
        in_specs=[heads, heads, rows, rows, full((t, N)), full((t, N))] + [anywhere] * 5,
        out_specs=[heads, rows, full((nb, L, L)), anywhere, anywhere, anywhere],
        out_shape=[jax.ShapeDtypeStruct((H, PD, t), F32), jax.ShapeDtypeStruct((H, t), F32), jax.ShapeDtypeStruct((nb, L, L), F32), state, state, state],
        scratch_shapes=[pltpu.VMEM((nb, L, L), F32), pltpu.VMEM((GD, H, L), F32), whole, halves] + [quarter] * 7 + [halves, whole, pltpu.VMEM((L, 2 * HG * L), BF16), pltpu.VMEM((2 * HG * L, L), BF16),
                           pltpu.VMEM((QR, N), F32), pltpu.VMEM((QR, N), F32)]
                       + [sems(5), sems(GD), sems(GD), sems(2, 2), sems(2, 2)] + [sems(2, QH)] * 6 + [sems(2, 2, QH)] * 2 + [sems(QH)] * 4 + [sems(2, QH)] * 2 + [sems(4)],
        compiler_params=pltpu.CompilerParams(dimension_semantics=("arbitrary",), collective_id=0, has_side_effects=True),
        cost_estimate=pl.CostEstimate(flops=10 ** 10, bytes_accessed=10 ** 7, transcendentals=0),
        name="chain_and_blocks",
    )(x, dy, dt, cs, b, c, tot, s_loc, g_loc, s0, g0)


def carried_kernel(x_ref, dy_ref, dt_ref, cs_ref, dui_ref, rs_ref, s0_ref, g1_ref, b_ref, c_ref, par_ref, dta_ref, para_ref, dg_ref,
                   dx_ref, ddt_ref, db_ref, dc_ref, dh_ref,
                   sf, gc, tu, sd, gh, us, db_acc, dc_acc, ec_s, td_s, tl_s, ddir_s, xd_s, dcs_s, kd_s, bb_ref, cc_ref, b2t_ref, ct_ref):
    nb = x_ref.shape[2] // L
    g = pl.program_id(0)

    @pl.when(g == 0)
    def _():
        for b in range(nb):
            bb, cc = b_ref[b * L:(b + 1) * L, :], c_ref[b * L:(b + 1) * L, :]
            bb_ref[b] = jnp.concatenate([bb, bb], axis=0)
            cc_ref[b] = jnp.concatenate([cc, cc], axis=0)
            bt = jnp.transpose(bb.astype(F32)).astype(BF16)
            b2t_ref[b] = jnp.concatenate([bt, bt], axis=0)
            ct_ref[b] = jnp.transpose(cc.astype(F32))
        db_acc[...] = jnp.zeros_like(db_acc)
        dc_acc[...] = jnp.zeros_like(dc_acc)

    heads = pl.ds(pl.multiple_of(g * HG, HG), HG)
    for b in range(nb):
        sl = slice(b * L, (b + 1) * L)
        cs = cs_ref[:, sl]
        tail = jnp.exp2(cs[:, L - 1:L] - cs)
        ec_s[b] = jnp.exp2(cs)
        tl_s[b] = tail
        td_s[b] = tail * dt_ref[:, sl]

    sf[0] = s0_ref[...]

    def forward(b, _):
        toks = pl.ds(pl.multiple_of(b * L, L), L)
        etot = ec_s[b][:, L - 1:L]
        td = td_s[b]
        for j in range(HG):
            hi, lo = split(x_ref[j, :, toks].astype(F32) * td[j:j + 1])
            tu[b, j * PD:(j + 1) * PD, :L] = hi
            tu[b, j * PD:(j + 1) * PD, L:] = lo
        new = dot(tu[b], bb_ref[b])
        for j in range(HG):
            pr = slice(j * PD, (j + 1) * PD)
            sf[b + 1, pr] = etot[j:j + 1] * sf[b, pr] + new[pr]
        return 0

    lax.fori_loop(0, nb, forward, 0)
    gc[...] = g1_ref[...]

    def backward(i, _):
        b = nb - 1 - i
        toks = pl.ds(pl.multiple_of(b * L, L), L)
        ec, tl, dtb = ec_s[b], tl_s[b], dt_ref[:, toks]
        etot = ec[:, L - 1:L]
        kd = []
        for j in range(HG):
            pr = slice(j * PD, (j + 1) * PD)
            gj = gc[pr]
            kd.append(jnp.sum(gj * sf[b + 1, pr], axis=0, keepdims=True))
            hi, lo = split(gj)
            gh[pr, :L] = hi
            gh[pr, L:] = lo
            hi, lo = split(dy_ref[j, :, toks].astype(F32) * ec[j:j + 1])
            sd[pr, :L] = hi
            sd[pr, L:] = lo
        kd_s[b, heads] = jnp.concatenate(kd, axis=0)
        us[...] = dot(gh[...], b2t_ref[b])
        db_acc[b] += (dot(gh[:, :L], tu[b, :, :L], TN) + dot(gh[:, L:], tu[b, :, :L], TN)) + dot(gh[:, :L], tu[b, :, L:], TN)
        ct = ct_ref[b]
        dc = jnp.zeros((N, L), F32)
        ddir, xd, inter = [], [], []
        for j in range(HG):
            pr = slice(j * PD, (j + 1) * PD)
            du = dui_ref[j, :, toks] + us[pr] * tl[j:j + 1]
            xf, dyf = x_ref[j, :, toks].astype(F32), dy_ref[j, :, toks].astype(F32)
            ddir.append(jnp.sum(du * xf, axis=0, keepdims=True))
            xd.append(jnp.sum(dyf * xf, axis=0, keepdims=True))
            dx_ref[j, :, toks] = (du * dtb[j:j + 1] + dyf * par_ref[j:j + 1, 1:2]).astype(BF16)
            shi, slo = split(sf[b, pr])
            st = jnp.transpose(jnp.concatenate([shi, slo], axis=0))
            st = jnp.concatenate([st, st], axis=1)
            dhi, dlo = sd[pr, :L], sd[pr, L:]
            z = dot(st, jnp.concatenate([dhi, dhi, dlo, dlo], axis=0))
            dc = dc + z
            inter.append(jnp.sum(z * ct, axis=0, keepdims=True))
        dc_acc[b] += dc
        ddir = jnp.concatenate(ddir, axis=0)
        ddir_s[b, heads] = ddir
        xd_s[b, heads] = jnp.concatenate(xd, axis=0)
        dcs_s[b, heads] = rs_ref[:, toks] + jnp.concatenate(inter, axis=0) - ddir * dtb
        grow = dot(sd[...], cc_ref[b])
        for j in range(HG):
            pr = slice(j * PD, (j + 1) * PD)
            gc[pr] = etot[j:j + 1] * gc[pr] + grow[pr]
        return 0

    lax.fori_loop(0, nb, backward, 0)

    @pl.when(g == pl.num_programs(0) - 1)
    def _():
        after = (lax.broadcasted_iota(jnp.int32, (L, L), 0) >= lax.broadcasted_iota(jnp.int32, (L, L), 1)).astype(F32)
        da_sum = jnp.zeros((H, 1), F32)
        dd_sum = jnp.zeros((H, 1), F32)
        for b in range(nb):
            sl = slice(b * L, (b + 1) * L)
            da = dot(dcs_s[b], after, precision=HIGHEST) + jnp.sum(kd_s[b], axis=1, keepdims=True)
            dta = da * para_ref[:, 0:1]
            ddt_ref[:, sl] = ddir_s[b] + dta
            da_sum += jnp.sum(dta * dta_ref[:, sl], axis=1, keepdims=True)
            dd_sum += jnp.sum(xd_s[b], axis=1, keepdims=True)
            ghi, glo = split(dg_ref[b])
            dbt = jnp.transpose(db_acc[b]) + (dot(ghi, cc_ref[b, :L, :], TN) + dot(glo, cc_ref[b, :L, :], TN))
            dct = jnp.transpose(dc_acc[b]) + (dot(ghi, bb_ref[b, :L, :]) + dot(glo, bb_ref[b, :L, :]))
            db_ref[sl, :] = dbt.astype(BF16)
            dc_ref[sl, :] = dct.astype(BF16)
        lane_h = lax.broadcasted_iota(jnp.int32, (H, L), 1)
        dh_ref[...] = jnp.where(lane_h == 0, da_sum, jnp.where(lane_h == 1, dd_sum, 0.0))


def carried(x, dy, dt, cs, dui, rs, s_start, ds_end, b, c, par, dg):
    t = x.shape[2]
    nb = t // L
    full = lambda shape: pl.BlockSpec(shape, lambda g: (0,) * len(shape))
    heads = pl.BlockSpec((HG, PD, t), lambda g: (g, 0, 0))
    rows = pl.BlockSpec((HG, t), lambda g: (g, 0))
    state = pl.BlockSpec((HG * PD, N), lambda g: (g, 0))
    one = pl.BlockSpec((HG, L), lambda g: (g, 0))
    vm = lambda shape, dtype=F32: pltpu.VMEM(shape, dtype)
    return pl.pallas_call(
        carried_kernel,
        grid=(H // HG,),
        in_specs=[heads, heads, rows, rows, heads, rows, state, state, full((t, N)), full((t, N)), one, full((H, t)), full((H, L)),
                  full((nb, L, L))],
        out_specs=[heads, full((H, t)), full((t, N)), full((t, N)), full((H, L))],
        out_shape=[jax.ShapeDtypeStruct((H, PD, t), BF16), jax.ShapeDtypeStruct((H, t), F32), jax.ShapeDtypeStruct((t, N), BF16),
                   jax.ShapeDtypeStruct((t, N), BF16), jax.ShapeDtypeStruct((H, L), F32)],
        scratch_shapes=[vm((nb + 1, HG * PD, N)), vm((HG * PD, N)), vm((nb, HG * PD, 2 * L), BF16), vm((HG * PD, 2 * L), BF16),
                        vm((HG * PD, 2 * N), BF16), vm((HG * PD, L)), vm((nb, N, L)), vm((nb, N, L)),
                        vm((nb, HG, L)), vm((nb, HG, L)), vm((nb, HG, L)), vm((nb, H, L)), vm((nb, H, L)), vm((nb, H, L)), vm((nb, H, N)),
                        vm((nb, 2 * L, N), BF16), vm((nb, 2 * L, N), BF16), vm((nb, 2 * N, L), BF16), vm((nb, N, L))],
        compiler_params=pltpu.CompilerParams(dimension_semantics=("arbitrary",)),
        cost_estimate=pl.CostEstimate(flops=5 * 10 ** 10, bytes_accessed=6 * H * PD * t, transcendentals=H * t * L),
        name="carried_backward",
    )(x, dy, dt, cs, dui, rs, s_start, ds_end, b, c, par, dt, par, dg)


def solution(mesh):
    nd = mesh.shape[AXIS]
    tok4 = P(None, AXIS, None, None)
    tok3 = P(None, AXIS, None)

    def device_step(x_loc, dt_loc, a_log, b_loc, c_loc, d_skip, s_init, dy_loc, ds_last):
        x, dy = jnp.transpose(x_loc[0], (1, 2, 0)), jnp.transpose(dy_loc[0], (1, 2, 0))
        dt = jnp.transpose(dt_loc[0])
        b, c = b_loc[0], c_loc[0]
        col = jnp.arange(L)[None, :]
        par = jnp.where(col == 0, -jnp.exp(a_log)[:, None], jnp.where(col == 1, d_skip[:, None], 0.0))
        s_loc, g_loc, cs, tot = summaries(x, dy, dt, par, b, c)
        s0, g0 = s_init.reshape(H * PD, N), ds_last.reshape(H * PD, N)
        dui, rs, dg, s_start, ds_end, first = chain_and_blocks(nd, x, dy, dt, cs, b, c, tot, s_loc, g_loc, s0, g0)
        dx, ddt, db, dc, dh = carried(x, dy, dt, cs, dui, rs, s_start, ds_end, b, c, par, dg)
        dh = tile_sum(nd, dh)
        return (jnp.transpose(dx, (2, 0, 1))[None], jnp.transpose(ddt)[None], db[None], dc[None], first.reshape(1, H, PD, N), dh[0, :H], dh[1, :H])

    return jax.shard_map(device_step, mesh=mesh,
                         in_specs=(tok4, tok3, P(), tok3, tok3, P(), P(), tok4, P()),
                         out_specs=(tok4, tok3, tok3, tok3, P(), P(), P()),
                         check_vma=False)
```

```python
import functools
import jax
import jax.numpy as jnp
from jax import lax
from jax.experimental import pallas as pl
from jax.experimental.pallas import tpu as pltpu
from jax.sharding import PartitionSpec as P

AXIS = 'cp'
H, PD, N = 80, 64, 128
L = 128
HG = 8
LOG2E = 1.4426950408889634
NEG = -1e30
F32, BF16 = jnp.float32, jnp.bfloat16
HIGHEST = lax.Precision.HIGHEST
NT = (((1,), (1,)), ((), ()))
TN = (((0,), (0,)), ((), ()))
NN = (((1,), (0,)), ((), ()))


def dot(a, b, dims=NN, precision=None):
    return lax.dot_general(a, b, dims, precision=precision, preferred_element_type=F32)


def split(v):
    hi = v.astype(BF16)
    return hi, (v - hi.astype(F32)).astype(BF16)


MESH = pl.DeviceIdType.MESH


def greet_all(nd, me):
    barrier = pltpu.get_barrier_semaphore()
    for o in range(1, nd):
        pl.semaphore_signal(barrier, inc=1, device_id=(lax.rem(me + o, nd),), device_id_type=MESH)
    pl.semaphore_wait(barrier, nd - 1)


def tile_copy(nd, me, o, got, send, recv):
    return pltpu.make_async_remote_copy(src_ref=got.at[me], dst_ref=got.at[me], send_sem=send.at[o], recv_sem=recv.at[o],
                                        device_id=(lax.rem(me + o, nd),), device_id_type=MESH)


def send_all(nd, me, got, send, recv):
    for o in range(1, nd):
        tile_copy(nd, me, o, got, send, recv).start()


def wait_all(nd, me, got, send, recv):
    for o in range(1, nd):
        src = lax.rem(me + nd - o, nd)
        pltpu.make_async_remote_copy(src_ref=got.at[src], dst_ref=got.at[src], send_sem=send.at[o], recv_sem=recv.at[o],
                                     device_id=(src,), device_id_type=MESH).wait_recv()
        tile_copy(nd, me, o, got, send, recv).wait_send()


def summary_kernel(x_ref, dy_ref, dt_ref, par_ref, b_ref, c_ref, s_ref, g_ref, cs_ref, tot_ref,
                   tu_hi, tu_lo, sd_hi, sd_lo, cs_all, off_all):
    nb = x_ref.shape[2] // L
    g = pl.program_id(0)

    @pl.when(g == 0)
    def _():
        tri = (lax.broadcasted_iota(jnp.int32, (L, L), 0) <= lax.broadcasted_iota(jnp.int32, (L, L), 1)).astype(F32)
        off = jnp.zeros((H, L), F32)
        for b in range(nb):
            sl = slice(b * L, (b + 1) * L)
            a = dt_ref[:, sl] * (par_ref[:, 0:1] * LOG2E)
            cs = dot(a, tri, precision=HIGHEST)
            cs_all[:, sl] = cs
            off_all[:, sl] = off
            off = off + jnp.broadcast_to(cs[:, L - 1:L], (H, L))
        off_all[:, nb * L:] = off
        cs_ref[...] = cs_all[...]
        tot_ref[...] = off

    rows = pl.ds(pl.multiple_of(g * HG, HG), HG)
    for b in range(nb):
        sl = slice(b * L, (b + 1) * L)
        run = cs_all[rows, sl] + off_all[rows, sl]
        ec = jnp.exp2(run)
        tl = jnp.exp2(off_all[rows, nb * L:] - run) * dt_ref[rows, sl]
        for j in range(HG):
            pr = slice(j * PD, (j + 1) * PD)
            tu_hi[pr, sl], tu_lo[pr, sl] = split(x_ref[j, :, sl].astype(F32) * tl[j:j + 1])
            sd_hi[pr, sl], sd_lo[pr, sl] = split(dy_ref[j, :, sl].astype(F32) * ec[j:j + 1])
    s_ref[...] = dot(tu_hi[...], b_ref[...]) + dot(tu_lo[...], b_ref[...])
    g_ref[...] = dot(sd_hi[...], c_ref[...]) + dot(sd_lo[...], c_ref[...])


def summaries(x, dy, dt, par, b, c):
    t = x.shape[2]
    full = lambda shape: pl.BlockSpec(shape, lambda g: (0,) * len(shape))
    heads = pl.BlockSpec((HG, PD, t), lambda g: (g, 0, 0))
    state = pl.BlockSpec((HG * PD, N), lambda g: (g, 0))
    half = pltpu.VMEM((HG * PD, t), BF16)
    return pl.pallas_call(
        summary_kernel,
        grid=(H // HG,),
        in_specs=[heads, heads, full((H, t)), full((H, L)), full((t, N)), full((t, N))],
        out_specs=[state, state, full((H, t)), full((H, L))],
        out_shape=[jax.ShapeDtypeStruct((H * PD, N), F32), jax.ShapeDtypeStruct((H * PD, N), F32),
                   jax.ShapeDtypeStruct((H, t), F32), jax.ShapeDtypeStruct((H, L), F32)],
        scratch_shapes=[half, half, half, half, pltpu.VMEM((H, t), F32), pltpu.VMEM((H, t + L), F32)],
        compiler_params=pltpu.CompilerParams(dimension_semantics=("arbitrary",)),
        cost_estimate=pl.CostEstimate(flops=4 * H * PD * N * t * 2, bytes_accessed=4 * H * PD * t, transcendentals=0),
        name="range_summaries",
    )(x, dy, dt, par, b, c)


def tile_sum_kernel(nd, dh_ref, out_ref, got, send, recv):
    me = lax.axis_index(AXIS)
    got[me] = jnp.transpose(jnp.concatenate([dh_ref[...], jnp.zeros((L - H, L), F32)], axis=0))[:8]
    greet_all(nd, me)
    send_all(nd, me, got, send, recv)
    wait_all(nd, me, got, send, recv)
    total = got[0]
    for d in range(1, nd):
        total = total + got[d]
    out_ref[...] = total


def tile_sum(nd, dh):
    vm = pl.BlockSpec(memory_space=pltpu.VMEM)
    return pl.pallas_call(
        functools.partial(tile_sum_kernel, nd),
        in_specs=[vm], out_specs=vm, out_shape=jax.ShapeDtypeStruct((8, L), F32),
        scratch_shapes=[pltpu.VMEM((nd, 8, L), F32), pltpu.SemaphoreType.DMA((nd,)), pltpu.SemaphoreType.DMA((nd,))],
        compiler_params=pltpu.CompilerParams(collective_id=2, has_side_effects=True),
        name="tile_sum",
    )(dh)


GD = 4
QH = H // GD
QR = QH * PD
F_BACK = 8
HOP = 3
BACK = 20


def chain_kernel(nd, x_ref, dy_ref, dt_ref, cs_ref, b_ref, c_ref, tot_ref, s_hbm, g_hbm, s0_ref, g0_ref,
                 dui_ref, rs_ref, dg_ref, s_end, g_end, first_ref,
                 gram, tots, own, par, tq, tx, xin, cin, cout, bsend, brecv, dsend, into, rsum, pick, fq, fxr, local_sem, tot_send, tot_recv, par_send, par_recv,
                 x_send, x_recv, c_send, c_recv, b_send, b_recv, d_send, d_recv, f_send, f_recv, fx_send, fx_recv, fd_send, fd_recv, out_sem):
    nb = x_ref.shape[2] // L
    ng = nd // GD
    g = pl.program_id(0)
    me = lax.axis_index(AXIS)
    q, core, chip, pos = lax.rem(me, 4), lax.rem(me, 2), lax.rem(me // 2, 2), me // 4
    other_core, other_chip = me + 1 - 2 * core, me + 2 - 4 * chip
    oq = lax.rem(q + 2, 4)
    local = (s_hbm, g_hbm)

    def rows(head, n=1):
        return pl.ds(pl.multiple_of(head * PD, PD), n * PD)

    def remote(src, dst, send, recv, to):
        return pltpu.make_async_remote_copy(src_ref=src, dst_ref=dst, send_sem=send, recv_sem=recv, device_id=(to,), device_id_type=MESH)

    def tot_copy(o):
        return remote(tot_ref, tots.at[q], tot_send.at[o], tot_recv.at[o], 4 * pos + lax.rem(q + o, 4))

    def tot_got(o):
        src = lax.rem(q + 4 - o, 4)
        return remote(tot_ref, tots.at[src], tot_send.at[o], tot_recv.at[o], 4 * pos + src)

    def par_copy(d, i):
        return remote(local[d].at[rows(QH * (2 * i + 1 - core), QH)], par.at[d, i], par_send.at[d, i], par_recv.at[d, i], other_core)

    def x_copy(d, k):
        return remote(tx.at[d, rows(k)], xin.at[d, rows(k)], x_send.at[d, k], x_recv.at[d, k], other_chip)

    def c_copy(d, k):
        return remote(cout.at[d, rows(k)], cin.at[d, rows(k)], c_send.at[d, k], c_recv.at[d, k], me + (4 - 8 * d))

    def b_copy(d, k):
        return remote(bsend.at[d, rows(k)], brecv.at[d, rows(k)], b_send.at[d, k], b_recv.at[d, k], other_chip)

    def d_copy(d, i, k):
        head = QH * (2 * i + core) + k
        return remote(dsend.at[d, i, rows(k)], into.at[d, rows(head)], d_send.at[d, i, k], d_recv.at[d, i, k], other_core)

    f_sends = ((lax.rem(pos, 2) == 0) & (pos < ng - 2), lax.rem(pos, 2) == 0)

    def f_copy(way, k):
        return remote(fq.at[rows(k)], fq.at[rows(k)], f_send.at[way, k], f_recv.at[k], me + (8 - 4 * way))

    def fx_copy(k):
        return remote(fq.at[rows(k)], fxr.at[rows(k)], fx_send.at[k], fx_recv.at[k], other_chip)

    def fd_copy(i, k):
        src, head = (fq, QH * q + k) if i == 0 else (fxr, QH * oq + k)
        return remote(src.at[rows(k)], first_ref.at[rows(head)], fd_send.at[i, k], fd_recv.at[i, k], other_core)

    def f_step(k):
        @pl.when(pos > 0)
        def _():
            f_copy(0, k).wait_recv()

        for way in range(2):
            @pl.when(f_sends[way])
            def _():
                f_copy(way, k).start()

        fx_copy(k).start()
        fd_copy(0, k).start()

    def f_back(k):
        fx_copy(k).wait_recv()
        fd_copy(1, k).start()

    def decay(qq, head):
        return tots[qq, pl.ds(head, 1), :]

    def core_level(d, i, k, state):
        head = QH * (2 * i + core) + k
        mine_near = core == d
        near = jnp.where(mine_near, own[d, rows(head)], par[d, i, rows(k)])
        e_near = jnp.exp2(decay(2 * chip + d, head))
        far = e_near * state + near
        into[d, rows(head)] = jnp.where(mine_near, state, far)
        dsend[d, i, rows(k)] = jnp.where(mine_near, far, state)
        d_copy(d, i, k).start()

    def chain_step(d, k):
        head = QH * q + k
        has_prev = (pos > 0) if d == 0 else (pos < ng - 1)
        has_next = (pos < ng - 1) if d == 0 else (pos > 0)
        x_copy(d, k).wait_recv()

        @pl.when(has_prev)
        def _():
            c_copy(d, k).wait_recv()

        mine_near = chip == d
        state = cin[d, rows(k)]
        near = jnp.where(mine_near, tq[d, rows(k)], xin[d, rows(k)])
        afar = jnp.where(mine_near, xin[d, rows(k)], tq[d, rows(k)])
        e_near = jnp.exp2(decay(2 * d, head) + decay(2 * d + 1, head))
        e_far = jnp.exp2(decay(2 - 2 * d, head) + decay(3 - 2 * d, head))
        far = e_near * state + near
        out = e_far * far + afar
        cout[d, rows(k)] = out

        if d == 1:
            @pl.when(pos == 0)
            def _():
                fq[rows(k)] = out

        @pl.when(has_next)
        def _():
            c_copy(d, k).start()

        bsend[d, rows(k)] = jnp.where(mine_near, far, state)
        b_copy(d, k).start()
        core_level(d, chip, k, jnp.where(mine_near, state, far))

    def back_step(d, k):
        b_copy(d, k).wait_recv()
        core_level(d, 1 - chip, k, brecv[d, rows(k)])

    def slot(n):
        for d in range(2):
            k = n - HOP * (pos if d == 0 else ng - 1 - pos)

            @pl.when((k >= 0) & (k < QH))
            def _():
                chain_step(d, k)

            @pl.when((k >= BACK) & (k < QH + BACK))
            def _():
                back_step(d, k - BACK)

        kf = n - (HOP * (ng - 1 + pos // 2 + lax.rem(pos, 2)) + 1)

        @pl.when((kf >= 0) & (kf < QH))
        def _():
            f_step(kf)

        @pl.when((kf >= F_BACK) & (kf < QH + F_BACK))
        def _():
            f_back(kf - F_BACK)

    @pl.when(g == 0)
    def _():
        locals_ = [pltpu.make_async_copy(s_hbm, own.at[0], local_sem.at[0]), pltpu.make_async_copy(g_hbm, own.at[1], local_sem.at[1]),
                   pltpu.make_async_copy(tot_ref, tots.at[q], local_sem.at[2]),
                   pltpu.make_async_copy(s0_ref.at[rows(QH * q, QH)], cin.at[0], local_sem.at[3]),
                   pltpu.make_async_copy(g0_ref.at[rows(QH * q, QH)], cin.at[1], local_sem.at[4])]
        for cp in locals_[:3]:
            cp.start()

        @pl.when(pos == 0)
        def _():
            locals_[3].start()
            locals_[3].wait()

        @pl.when(pos == ng - 1)
        def _():
            locals_[4].start()
            locals_[4].wait()

        greet_all(nd, me)
        for o in range(1, GD):
            tot_copy(o).start()
        for d in range(2):
            for i in range(2):
                par_copy(d, i).start()
        for b in range(nb):
            sl = slice(b * L, (b + 1) * L)
            gram[b] = dot(c_ref[sl, :], b_ref[sl, :], NT)
        dg_ref[...] = jnp.zeros_like(dg_ref)
        for j in range(2 * HG):
            pick[j * L:(j + 1) * L, :] = (lax.broadcasted_iota(jnp.int32, (L, L), 1) == j // 2).astype(F32).astype(BF16)
        for cp in locals_[:3]:
            cp.wait()
        for o in range(1, GD):
            tot_got(o).wait_recv()
        for d in range(2):
            for i in range(2):
                par_copy(d, i).wait_recv()

        def combine(d, i, k):
            head = QH * (2 * i + core) + k
            mine_near = core == d
            mine, his = own[d, rows(head)], par[d, i, rows(k)]
            e_far = jnp.exp2(decay(2 * chip + 1 - d, head))
            return e_far * jnp.where(mine_near, mine, his) + jnp.where(mine_near, his, mine)

        def front(turn, k, _):
            for d in range(2):
                @pl.when((turn == d) == (pos < ng // 2))
                def _():
                    tx[d, rows(k)] = combine(d, 1 - chip, k)
                    x_copy(d, k).start()
                    tq[d, rows(k)] = combine(d, chip, k)
            return 0

        for turn in (0, 1):
            lax.fori_loop(0, QH, functools.partial(front, turn), 0)

    below = lax.broadcasted_iota(jnp.int32, (L, L), 0) >= lax.broadcasted_iota(jnp.int32, (L, L), 1)

    def work(b, _):
        slot(g * nb + b)
        toks = pl.ds(pl.multiple_of(b * L, L), L)
        cs, dtb = cs_ref[:, toks], dt_ref[:, toks]
        cst = jnp.transpose(cs)
        gram_b = gram[b]
        dg = jnp.zeros((L, L), F32)
        for j in range(HG):
            xj, dyj = x_ref[j, :, toks], dy_ref[j, :, toks]
            e = jnp.exp2(jnp.where(below, jnp.broadcast_to(cst[:, j:j + 1], (L, L)) - cs[j:j + 1], NEG))
            mhi, mlo = split(gram_b * e)
            dui_ref[j, :, toks] = dot(jnp.concatenate([dyj, dyj], axis=1), jnp.concatenate([mhi, mlo], axis=0))
            w = dot(dyj, xj, TN) * (e * dtb[j:j + 1])
            dg = dg + w
            rsum[:, (2 * j) * L:(2 * j + 1) * L], rsum[:, (2 * j + 1) * L:(2 * j + 2) * L] = split(w * gram_b)
        dg_ref[b] += dg
        rs_ref[:, toks] = jnp.transpose(dot(rsum[...], pick[...]))[:HG]
        return 0

    lax.fori_loop(0, nb, work, 0)

    @pl.when(g == pl.num_programs(0) - 1)
    def _():
        def rest(n, _):
            slot(n)
            return 0

        lax.fori_loop((H // HG) * nb, max(HOP * (ng - 1) + BACK, HOP * (ng - 1 + ng // 2) + 1 + F_BACK) + QH, rest, 0)

        def drain(k, _):
            for d in range(2):
                x_copy(d, k).wait_send()
                b_copy(d, k).wait_send()

                @pl.when((pos < ng - 1) if d == 0 else (pos > 0))
                def _():
                    c_copy(d, k).wait_send()

                for i in range(2):
                    d_copy(d, i, k).wait()

            for way in range(2):
                @pl.when(f_sends[way])
                def _():
                    f_copy(way, k).wait_send()

            fx_copy(k).wait_send()
            for i in range(2):
                fd_copy(i, k).wait()
            return 0

        early = [pltpu.make_async_copy(fq, first_ref.at[rows(QH * q, QH)], out_sem.at[2]),
                 pltpu.make_async_copy(fxr, first_ref.at[rows(QH * oq, QH)], out_sem.at[3])]
        for out in early:
            out.start()
        lax.fori_loop(0, QH, drain, 0)
        outs = [pltpu.make_async_copy(into.at[0], s_end, out_sem.at[0]), pltpu.make_async_copy(into.at[1], g_end, out_sem.at[1])]
        for out in outs:
            out.start()
        for o in range(1, GD):
            tot_copy(o).wait_send()
        for d in range(2):
            for i in range(2):
                par_copy(d, i).wait_send()
        for out in early + outs:
            out.wait()


def chain_and_blocks(nd, x, dy, dt, cs, b, c, tot, s_loc, g_loc, s0, g0):
    t = x.shape[2]
    nb = t // L
    full = lambda shape: pl.BlockSpec(shape, lambda g: (0,) * len(shape))
    heads = pl.BlockSpec((HG, PD, t), lambda g: (g, 0, 0))
    rows = pl.BlockSpec((HG, t), lambda g: (g, 0))
    anywhere = pl.BlockSpec(memory_space=pl.ANY)
    quarter = pltpu.VMEM((2, QR, N), F32)
    whole = pltpu.VMEM((2, H * PD, N), F32)
    halves = pltpu.VMEM((2, 2, QR, N), F32)
    sems = lambda *shape: pltpu.SemaphoreType.DMA(shape)
    state = jax.ShapeDtypeStruct((H * PD, N), F32)
    return pl.pallas_call(
        functools.partial(chain_kernel, nd),
        grid=(H // HG,),
        in_specs=[heads, heads, rows, rows, full((t, N)), full((t, N))] + [anywhere] * 5,
        out_specs=[heads, rows, full((nb, L, L)), anywhere, anywhere, anywhere],
        out_shape=[jax.ShapeDtypeStruct((H, PD, t), F32), jax.ShapeDtypeStruct((H, t), F32), jax.ShapeDtypeStruct((nb, L, L), F32), state, state, state],
        scratch_shapes=[pltpu.VMEM((nb, L, L), F32), pltpu.VMEM((GD, H, L), F32), whole, halves] + [quarter] * 7 + [halves, whole, pltpu.VMEM((L, 2 * HG * L), BF16), pltpu.VMEM((2 * HG * L, L), BF16),
                           pltpu.VMEM((QR, N), F32), pltpu.VMEM((QR, N), F32)]
                       + [sems(5), sems(GD), sems(GD), sems(2, 2), sems(2, 2)] + [sems(2, QH)] * 6 + [sems(2, 2, QH)] * 2 + [sems(2, QH)] + [sems(QH)] * 3 + [sems(2, QH)] * 2 + [sems(4)],
        compiler_params=pltpu.CompilerParams(dimension_semantics=("arbitrary",), collective_id=0, has_side_effects=True),
        cost_estimate=pl.CostEstimate(flops=10 ** 10, bytes_accessed=10 ** 7, transcendentals=0),
        name="chain_and_blocks",
    )(x, dy, dt, cs, b, c, tot, s_loc, g_loc, s0, g0)


def carried_kernel(x_ref, dy_ref, dt_ref, cs_ref, dui_ref, rs_ref, s0_ref, g1_ref, b_ref, c_ref, par_ref, dta_ref, para_ref, dg_ref,
                   dx_ref, ddt_ref, db_ref, dc_ref, dh_ref,
                   sf, gc, tu, sd, gh, us, db_acc, dc_acc, ec_s, td_s, tl_s, ddir_s, xd_s, dcs_s, kd_s, bb_ref, cc_ref, b2t_ref, ct_ref):
    nb = x_ref.shape[2] // L
    g = pl.program_id(0)

    @pl.when(g == 0)
    def _():
        for b in range(nb):
            bb, cc = b_ref[b * L:(b + 1) * L, :], c_ref[b * L:(b + 1) * L, :]
            bb_ref[b] = jnp.concatenate([bb, bb], axis=0)
            cc_ref[b] = jnp.concatenate([cc, cc], axis=0)
            bt = jnp.transpose(bb.astype(F32)).astype(BF16)
            b2t_ref[b] = jnp.concatenate([bt, bt], axis=0)
            ct_ref[b] = jnp.transpose(cc.astype(F32))
        db_acc[...] = jnp.zeros_like(db_acc)
        dc_acc[...] = jnp.zeros_like(dc_acc)

    heads = pl.ds(pl.multiple_of(g * HG, HG), HG)
    for b in range(nb):
        sl = slice(b * L, (b + 1) * L)
        cs = cs_ref[:, sl]
        tail = jnp.exp2(cs[:, L - 1:L] - cs)
        ec_s[b] = jnp.exp2(cs)
        tl_s[b] = tail
        td_s[b] = tail * dt_ref[:, sl]

    sf[0] = s0_ref[...]

    def forward(b, _):
        toks = pl.ds(pl.multiple_of(b * L, L), L)
        etot = ec_s[b][:, L - 1:L]
        td = td_s[b]
        for j in range(HG):
            hi, lo = split(x_ref[j, :, toks].astype(F32) * td[j:j + 1])
            tu[b, j * PD:(j + 1) * PD, :L] = hi
            tu[b, j * PD:(j + 1) * PD, L:] = lo
        new = dot(tu[b], bb_ref[b])
        for j in range(HG):
            pr = slice(j * PD, (j + 1) * PD)
            sf[b + 1, pr] = etot[j:j + 1] * sf[b, pr] + new[pr]
        return 0

    lax.fori_loop(0, nb, forward, 0)
    gc[...] = g1_ref[...]

    def backward(i, _):
        b = nb - 1 - i
        toks = pl.ds(pl.multiple_of(b * L, L), L)
        ec, tl, dtb = ec_s[b], tl_s[b], dt_ref[:, toks]
        etot = ec[:, L - 1:L]
        kd = []
        for j in range(HG):
            pr = slice(j * PD, (j + 1) * PD)
            gj = gc[pr]
            kd.append(jnp.sum(gj * sf[b + 1, pr], axis=0, keepdims=True))
            hi, lo = split(gj)
            gh[pr, :L] = hi
            gh[pr, L:] = lo
            hi, lo = split(dy_ref[j, :, toks].astype(F32) * ec[j:j + 1])
            sd[pr, :L] = hi
            sd[pr, L:] = lo
        kd_s[b, heads] = jnp.concatenate(kd, axis=0)
        us[...] = dot(gh[...], b2t_ref[b])
        wide = dot(gh[...], tu[b], TN)
        db_acc[b] += (wide[:N, :L] + wide[:N, L:]) + (wide[N:, :L] + wide[N:, L:])
        ct = ct_ref[b]
        dc = jnp.zeros((N, L), F32)
        ddir, xd, inter = [], [], []
        for j in range(HG):
            pr = slice(j * PD, (j + 1) * PD)
            du = dui_ref[j, :, toks] + us[pr] * tl[j:j + 1]
            xf, dyf = x_ref[j, :, toks].astype(F32), dy_ref[j, :, toks].astype(F32)
            ddir.append(jnp.sum(du * xf, axis=0, keepdims=True))
            xd.append(jnp.sum(dyf * xf, axis=0, keepdims=True))
            dx_ref[j, :, toks] = (du * dtb[j:j + 1] + dyf * par_ref[j:j + 1, 1:2]).astype(BF16)
            shi, slo = split(sf[b, pr])
            st = jnp.transpose(jnp.concatenate([shi, slo], axis=0))
            st = jnp.concatenate([st, st], axis=1)
            dhi, dlo = sd[pr, :L], sd[pr, L:]
            z = dot(st, jnp.concatenate([dhi, dhi, dlo, dlo], axis=0))
            dc = dc + z
            inter.append(jnp.sum(z * ct, axis=0, keepdims=True))
        dc_acc[b] += dc
        ddir = jnp.concatenate(ddir, axis=0)
        ddir_s[b, heads] = ddir
        xd_s[b, heads] = jnp.concatenate(xd, axis=0)
        dcs_s[b, heads] = rs_ref[:, toks] + jnp.concatenate(inter, axis=0) - ddir * dtb
        grow = dot(sd[...], cc_ref[b])
        for j in range(HG):
            pr = slice(j * PD, (j + 1) * PD)
            gc[pr] = etot[j:j + 1] * gc[pr] + grow[pr]
        return 0

    lax.fori_loop(0, nb, backward, 0)

    @pl.when(g == pl.num_programs(0) - 1)
    def _():
        after = (lax.broadcasted_iota(jnp.int32, (L, L), 0) >= lax.broadcasted_iota(jnp.int32, (L, L), 1)).astype(F32)
        da_sum = jnp.zeros((H, 1), F32)
        dd_sum = jnp.zeros((H, 1), F32)
        for b in range(nb):
            sl = slice(b * L, (b + 1) * L)
            da = dot(dcs_s[b], after, precision=HIGHEST) + jnp.sum(kd_s[b], axis=1, keepdims=True)
            dta = da * para_ref[:, 0:1]
            ddt_ref[:, sl] = ddir_s[b] + dta
            da_sum += jnp.sum(dta * dta_ref[:, sl], axis=1, keepdims=True)
            dd_sum += jnp.sum(xd_s[b], axis=1, keepdims=True)
            ghi, glo = split(dg_ref[b])
            dbt = jnp.transpose(db_acc[b]) + (dot(ghi, cc_ref[b, :L, :], TN) + dot(glo, cc_ref[b, :L, :], TN))
            dct = jnp.transpose(dc_acc[b]) + (dot(ghi, bb_ref[b, :L, :]) + dot(glo, bb_ref[b, :L, :]))
            db_ref[sl, :] = dbt.astype(BF16)
            dc_ref[sl, :] = dct.astype(BF16)
        lane_h = lax.broadcasted_iota(jnp.int32, (H, L), 1)
        dh_ref[...] = jnp.where(lane_h == 0, da_sum, jnp.where(lane_h == 1, dd_sum, 0.0))


def carried(x, dy, dt, cs, dui, rs, s_start, ds_end, b, c, par, dg):
    t = x.shape[2]
    nb = t // L
    full = lambda shape: pl.BlockSpec(shape, lambda g: (0,) * len(shape))
    heads = pl.BlockSpec((HG, PD, t), lambda g: (g, 0, 0))
    rows = pl.BlockSpec((HG, t), lambda g: (g, 0))
    state = pl.BlockSpec((HG * PD, N), lambda g: (g, 0))
    one = pl.BlockSpec((HG, L), lambda g: (g, 0))
    vm = lambda shape, dtype=F32: pltpu.VMEM(shape, dtype)
    return pl.pallas_call(
        carried_kernel,
        grid=(H // HG,),
        in_specs=[heads, heads, rows, rows, heads, rows, state, state, full((t, N)), full((t, N)), one, full((H, t)), full((H, L)),
                  full((nb, L, L))],
        out_specs=[heads, full((H, t)), full((t, N)), full((t, N)), full((H, L))],
        out_shape=[jax.ShapeDtypeStruct((H, PD, t), BF16), jax.ShapeDtypeStruct((H, t), F32), jax.ShapeDtypeStruct((t, N), BF16),
                   jax.ShapeDtypeStruct((t, N), BF16), jax.ShapeDtypeStruct((H, L), F32)],
        scratch_shapes=[vm((nb + 1, HG * PD, N)), vm((HG * PD, N)), vm((nb, HG * PD, 2 * L), BF16), vm((HG * PD, 2 * L), BF16),
                        vm((HG * PD, 2 * N), BF16), vm((HG * PD, L)), vm((nb, N, L)), vm((nb, N, L)),
                        vm((nb, HG, L)), vm((nb, HG, L)), vm((nb, HG, L)), vm((nb, H, L)), vm((nb, H, L)), vm((nb, H, L)), vm((nb, H, N)),
                        vm((nb, 2 * L, N), BF16), vm((nb, 2 * L, N), BF16), vm((nb, 2 * N, L), BF16), vm((nb, N, L))],
        compiler_params=pltpu.CompilerParams(dimension_semantics=("arbitrary",)),
        cost_estimate=pl.CostEstimate(flops=5 * 10 ** 10, bytes_accessed=6 * H * PD * t, transcendentals=H * t * L),
        name="carried_backward",
    )(x, dy, dt, cs, dui, rs, s_start, ds_end, b, c, par, dt, par, dg)


def solution(mesh):
    nd = mesh.shape[AXIS]
    tok4 = P(None, AXIS, None, None)
    tok3 = P(None, AXIS, None)

    def device_step(x_loc, dt_loc, a_log, b_loc, c_loc, d_skip, s_init, dy_loc, ds_last):
        x, dy = jnp.transpose(x_loc[0], (1, 2, 0)), jnp.transpose(dy_loc[0], (1, 2, 0))
        dt = jnp.transpose(dt_loc[0])
        b, c = b_loc[0], c_loc[0]
        col = jnp.arange(L)[None, :]
        par = jnp.where(col == 0, -jnp.exp(a_log)[:, None], jnp.where(col == 1, d_skip[:, None], 0.0))
        s_loc, g_loc, cs, tot = summaries(x, dy, dt, par, b, c)
        s0, g0 = s_init.reshape(H * PD, N), ds_last.reshape(H * PD, N)
        dui, rs, dg, s_start, ds_end, first = chain_and_blocks(nd, x, dy, dt, cs, b, c, tot, s_loc, g_loc, s0, g0)
        dx, ddt, db, dc, dh = carried(x, dy, dt, cs, dui, rs, s_start, ds_end, b, c, par, dg)
        dh = tile_sum(nd, dh)
        return (jnp.transpose(dx, (2, 0, 1))[None], jnp.transpose(ddt)[None], db[None], dc[None], first.reshape(1, H, PD, N), dh[0, :H], dh[1, :H])

    return jax.shard_map(device_step, mesh=mesh,
                         in_specs=(tok4, tok3, P(), tok3, tok3, P(), P(), tok4, P()),
                         out_specs=(tok4, tok3, tok3, tok3, P(), P(), P()),
                         check_vma=False)
```

```python
import functools
import jax
import jax.numpy as jnp
from jax import lax
from jax.experimental import pallas as pl
from jax.experimental.pallas import tpu as pltpu
from jax.sharding import PartitionSpec as P

AXIS = 'cp'
H, PD, N = 80, 64, 128
L = 128
HG = 8
LOG2E = 1.4426950408889634
NEG = -1e30
F32, BF16 = jnp.float32, jnp.bfloat16
HIGHEST = lax.Precision.HIGHEST
NT = (((1,), (1,)), ((), ()))
TN = (((0,), (0,)), ((), ()))
NN = (((1,), (0,)), ((), ()))


def dot(a, b, dims=NN, precision=None):
    return lax.dot_general(a, b, dims, precision=precision, preferred_element_type=F32)


def split(v):
    hi = v.astype(BF16)
    return hi, (v - hi.astype(F32)).astype(BF16)


MESH = pl.DeviceIdType.MESH


def greet_all(nd, me):
    barrier = pltpu.get_barrier_semaphore()
    for o in range(1, nd):
        pl.semaphore_signal(barrier, inc=1, device_id=(lax.rem(me + o, nd),), device_id_type=MESH)
    pl.semaphore_wait(barrier, nd - 1)


def tile_copy(nd, me, o, got, send, recv):
    return pltpu.make_async_remote_copy(src_ref=got.at[me], dst_ref=got.at[me], send_sem=send.at[o], recv_sem=recv.at[o],
                                        device_id=(lax.rem(me + o, nd),), device_id_type=MESH)


def send_all(nd, me, got, send, recv):
    for o in range(1, nd):
        tile_copy(nd, me, o, got, send, recv).start()


def wait_all(nd, me, got, send, recv):
    for o in range(1, nd):
        src = lax.rem(me + nd - o, nd)
        pltpu.make_async_remote_copy(src_ref=got.at[src], dst_ref=got.at[src], send_sem=send.at[o], recv_sem=recv.at[o],
                                     device_id=(src,), device_id_type=MESH).wait_recv()
        tile_copy(nd, me, o, got, send, recv).wait_send()


def summary_kernel(x_ref, dy_ref, dt_ref, par_ref, b_ref, c_ref, s_ref, g_ref, cs_ref, tot_ref,
                   tu_hi, tu_lo, sd_hi, sd_lo, cs_all, off_all):
    nb = x_ref.shape[2] // L
    g = pl.program_id(0)

    @pl.when(g == 0)
    def _():
        tri = (lax.broadcasted_iota(jnp.int32, (L, L), 0) <= lax.broadcasted_iota(jnp.int32, (L, L), 1)).astype(F32)
        off = jnp.zeros((H, L), F32)
        for b in range(nb):
            sl = slice(b * L, (b + 1) * L)
            a = dt_ref[:, sl] * (par_ref[:, 0:1] * LOG2E)
            cs = dot(a, tri, precision=HIGHEST)
            cs_all[:, sl] = cs
            off_all[:, sl] = off
            off = off + jnp.broadcast_to(cs[:, L - 1:L], (H, L))
        off_all[:, nb * L:] = off
        cs_ref[...] = cs_all[...]
        tot_ref[...] = off

    rows = pl.ds(pl.multiple_of(g * HG, HG), HG)
    for b in range(nb):
        sl = slice(b * L, (b + 1) * L)
        run = cs_all[rows, sl] + off_all[rows, sl]
        ec = jnp.exp2(run)
        tl = jnp.exp2(off_all[rows, nb * L:] - run) * dt_ref[rows, sl]
        for j in range(HG):
            pr = slice(j * PD, (j + 1) * PD)
            tu_hi[pr, sl], tu_lo[pr, sl] = split(x_ref[j, :, sl].astype(F32) * tl[j:j + 1])
            sd_hi[pr, sl], sd_lo[pr, sl] = split(dy_ref[j, :, sl].astype(F32) * ec[j:j + 1])
    s_ref[...] = dot(tu_hi[...], b_ref[...]) + dot(tu_lo[...], b_ref[...])
    g_ref[...] = dot(sd_hi[...], c_ref[...]) + dot(sd_lo[...], c_ref[...])


def summaries(x, dy, dt, par, b, c):
    t = x.shape[2]
    full = lambda shape: pl.BlockSpec(shape, lambda g: (0,) * len(shape))
    heads = pl.BlockSpec((HG, PD, t), lambda g: (g, 0, 0))
    state = pl.BlockSpec((HG * PD, N), lambda g: (g, 0))
    half = pltpu.VMEM((HG * PD, t), BF16)
    return pl.pallas_call(
        summary_kernel,
        grid=(H // HG,),
        in_specs=[heads, heads, full((H, t)), full((H, L)), full((t, N)), full((t, N))],
        out_specs=[state, state, full((H, t)), full((H, L))],
        out_shape=[jax.ShapeDtypeStruct((H * PD, N), F32), jax.ShapeDtypeStruct((H * PD, N), F32),
                   jax.ShapeDtypeStruct((H, t), F32), jax.ShapeDtypeStruct((H, L), F32)],
        scratch_shapes=[half, half, half, half, pltpu.VMEM((H, t), F32), pltpu.VMEM((H, t + L), F32)],
        compiler_params=pltpu.CompilerParams(dimension_semantics=("arbitrary",)),
        cost_estimate=pl.CostEstimate(flops=4 * H * PD * N * t * 2, bytes_accessed=4 * H * PD * t, transcendentals=0),
        name="range_summaries",
    )(x, dy, dt, par, b, c)


def tile_sum_kernel(nd, dh_ref, out_ref, got, send, recv):
    me = lax.axis_index(AXIS)
    got[me] = jnp.transpose(jnp.concatenate([dh_ref[...], jnp.zeros((L - H, L), F32)], axis=0))[:8]
    greet_all(nd, me)
    send_all(nd, me, got, send, recv)
    wait_all(nd, me, got, send, recv)
    total = got[0]
    for d in range(1, nd):
        total = total + got[d]
    out_ref[...] = total


def tile_sum(nd, dh):
    vm = pl.BlockSpec(memory_space=pltpu.VMEM)
    return pl.pallas_call(
        functools.partial(tile_sum_kernel, nd),
        in_specs=[vm], out_specs=vm, out_shape=jax.ShapeDtypeStruct((8, L), F32),
        scratch_shapes=[pltpu.VMEM((nd, 8, L), F32), pltpu.SemaphoreType.DMA((nd,)), pltpu.SemaphoreType.DMA((nd,))],
        compiler_params=pltpu.CompilerParams(collective_id=2, has_side_effects=True),
        name="tile_sum",
    )(dh)


GD = 4
QH = H // GD
QR = QH * PD
F_HOP = 5
F_BACK = 12
HOP = 3
BACK = 20


def chain_kernel(nd, x_ref, dy_ref, dt_ref, cs_ref, b_ref, c_ref, tot_ref, s_hbm, g_hbm, s0_ref, g0_ref,
                 dui_ref, rs_ref, dg_ref, s_end, g_end, first_ref,
                 gram, tots, own, par, tq, tx, xin, cin, cout, bsend, brecv, dsend, into, rsum, pick, fq, fxr, local_sem, tot_send, tot_recv, par_send, par_recv,
                 x_send, x_recv, c_send, c_recv, b_send, b_recv, d_send, d_recv, f_send, f_recv, fx_send, fx_recv, fd_send, fd_recv, out_sem):
    nb = x_ref.shape[2] // L
    ng = nd // GD
    g = pl.program_id(0)
    me = lax.axis_index(AXIS)
    q, core, chip, pos = lax.rem(me, 4), lax.rem(me, 2), lax.rem(me // 2, 2), me // 4
    other_core, other_chip = me + 1 - 2 * core, me + 2 - 4 * chip
    oq = lax.rem(q + 2, 4)
    local = (s_hbm, g_hbm)

    def rows(head, n=1):
        return pl.ds(pl.multiple_of(head * PD, PD), n * PD)

    def remote(src, dst, send, recv, to):
        return pltpu.make_async_remote_copy(src_ref=src, dst_ref=dst, send_sem=send, recv_sem=recv, device_id=(to,), device_id_type=MESH)

    def tot_copy(o):
        return remote(tot_ref, tots.at[q], tot_send.at[o], tot_recv.at[o], 4 * pos + lax.rem(q + o, 4))

    def tot_got(o):
        src = lax.rem(q + 4 - o, 4)
        return remote(tot_ref, tots.at[src], tot_send.at[o], tot_recv.at[o], 4 * pos + src)

    def par_copy(d, i):
        return remote(local[d].at[rows(QH * (2 * i + 1 - core), QH)], par.at[d, i], par_send.at[d, i], par_recv.at[d, i], other_core)

    def x_copy(d, k):
        return remote(tx.at[d, rows(k)], xin.at[d, rows(k)], x_send.at[d, k], x_recv.at[d, k], other_chip)

    def c_copy(d, k):
        return remote(cout.at[d, rows(k)], cin.at[d, rows(k)], c_send.at[d, k], c_recv.at[d, k], me + (4 - 8 * d))

    def b_copy(d, k):
        return remote(bsend.at[d, rows(k)], brecv.at[d, rows(k)], b_send.at[d, k], b_recv.at[d, k], other_chip)

    def d_copy(d, i, k):
        head = QH * (2 * i + core) + k
        return remote(dsend.at[d, i, rows(k)], into.at[d, rows(head)], d_send.at[d, i, k], d_recv.at[d, i, k], other_core)

    f_sends = ((lax.rem(pos, 2) == 0) & (pos < ng - 2), lax.rem(pos, 2) == 0)

    def f_copy(way, k):
        return remote(fq.at[rows(k)], fq.at[rows(k)], f_send.at[way, k], f_recv.at[k], me + (8 - 4 * way))

    def fx_copy(k):
        return remote(fq.at[rows(k)], fxr.at[rows(k)], fx_send.at[k], fx_recv.at[k], other_chip)

    def fd_copy(i, k):
        src, head = (fq, QH * q + k) if i == 0 else (fxr, QH * oq + k)
        return remote(src.at[rows(k)], first_ref.at[rows(head)], fd_send.at[i, k], fd_recv.at[i, k], other_core)

    def f_step(k):
        @pl.when(pos > 0)
        def _():
            f_copy(0, k).wait_recv()

        for way in range(2):
            @pl.when(f_sends[way])
            def _():
                f_copy(way, k).start()

        fx_copy(k).start()
        fd_copy(0, k).start()

    def f_back(k):
        fx_copy(k).wait_recv()
        fd_copy(1, k).start()

    def decay(qq, head):
        return tots[qq, pl.ds(head, 1), :]

    def core_level(d, i, k, state):
        head = QH * (2 * i + core) + k
        mine_near = core == d
        near = jnp.where(mine_near, own[d, rows(head)], par[d, i, rows(k)])
        e_near = jnp.exp2(decay(2 * chip + d, head))
        far = e_near * state + near
        into[d, rows(head)] = jnp.where(mine_near, state, far)
        dsend[d, i, rows(k)] = jnp.where(mine_near, far, state)
        d_copy(d, i, k).start()

    def chain_step(d, k):
        head = QH * q + k
        has_prev = (pos > 0) if d == 0 else (pos < ng - 1)
        has_next = (pos < ng - 1) if d == 0 else (pos > 0)
        x_copy(d, k).wait_recv()

        @pl.when(has_prev)
        def _():
            c_copy(d, k).wait_recv()

        mine_near = chip == d
        state = cin[d, rows(k)]
        near = jnp.where(mine_near, tq[d, rows(k)], xin[d, rows(k)])
        afar = jnp.where(mine_near, xin[d, rows(k)], tq[d, rows(k)])
        e_near = jnp.exp2(decay(2 * d, head) + decay(2 * d + 1, head))
        e_far = jnp.exp2(decay(2 - 2 * d, head) + decay(3 - 2 * d, head))
        far = e_near * state + near
        out = e_far * far + afar
        cout[d, rows(k)] = out

        if d == 1:
            @pl.when(pos == 0)
            def _():
                fq[rows(k)] = out

        @pl.when(has_next)
        def _():
            c_copy(d, k).start()

        bsend[d, rows(k)] = jnp.where(mine_near, far, state)
        b_copy(d, k).start()
        core_level(d, chip, k, jnp.where(mine_near, state, far))

    def back_step(d, k):
        b_copy(d, k).wait_recv()
        core_level(d, 1 - chip, k, brecv[d, rows(k)])

    def slot(n):
        for d in range(2):
            k = n - HOP * (pos if d == 0 else ng - 1 - pos)

            @pl.when((k >= 0) & (k < QH))
            def _():
                chain_step(d, k)

            @pl.when((k >= BACK) & (k < QH + BACK))
            def _():
                back_step(d, k - BACK)

        kf = n - (HOP * (ng - 1) + F_HOP * (pos // 2 + lax.rem(pos, 2)) + 1)

        @pl.when((kf >= 0) & (kf < QH))
        def _():
            f_step(kf)

        @pl.when((kf >= F_BACK) & (kf < QH + F_BACK))
        def _():
            f_back(kf - F_BACK)

    @pl.when(g == 0)
    def _():
        locals_ = [pltpu.make_async_copy(s_hbm, own.at[0], local_sem.at[0]), pltpu.make_async_copy(g_hbm, own.at[1], local_sem.at[1]),
                   pltpu.make_async_copy(tot_ref, tots.at[q], local_sem.at[2]),
                   pltpu.make_async_copy(s0_ref.at[rows(QH * q, QH)], cin.at[0], local_sem.at[3]),
                   pltpu.make_async_copy(g0_ref.at[rows(QH * q, QH)], cin.at[1], local_sem.at[4])]
        for cp in locals_[:3]:
            cp.start()

        @pl.when(pos == 0)
        def _():
            locals_[3].start()
            locals_[3].wait()

        @pl.when(pos == ng - 1)
        def _():
            locals_[4].start()
            locals_[4].wait()

        greet_all(nd, me)
        for o in range(1, GD):
            tot_copy(o).start()
        for d in range(2):
            for i in range(2):
                par_copy(d, i).start()
        for b in range(nb):
            sl = slice(b * L, (b + 1) * L)
            gram[b] = dot(c_ref[sl, :], b_ref[sl, :], NT)
        dg_ref[...] = jnp.zeros_like(dg_ref)
        for j in range(2 * HG):
            pick[j * L:(j + 1) * L, :] = (lax.broadcasted_iota(jnp.int32, (L, L), 1) == j // 2).astype(F32).astype(BF16)
        for cp in locals_[:3]:
            cp.wait()
        for o in range(1, GD):
            tot_got(o).wait_recv()
        for d in range(2):
            for i in range(2):
                par_copy(d, i).wait_recv()

        def combine(d, i, k):
            head = QH * (2 * i + core) + k
            mine_near = core == d
            mine, his = own[d, rows(head)], par[d, i, rows(k)]
            e_far = jnp.exp2(decay(2 * chip + 1 - d, head))
            return e_far * jnp.where(mine_near, mine, his) + jnp.where(mine_near, his, mine)

        def front(turn, k, _):
            for d in range(2):
                @pl.when((turn == d) == (pos < ng // 2))
                def _():
                    tx[d, rows(k)] = combine(d, 1 - chip, k)
                    x_copy(d, k).start()
                    tq[d, rows(k)] = combine(d, chip, k)
            return 0

        for turn in (0, 1):
            lax.fori_loop(0, QH, functools.partial(front, turn), 0)

    below = lax.broadcasted_iota(jnp.int32, (L, L), 0) >= lax.broadcasted_iota(jnp.int32, (L, L), 1)

    def work(b, _):
        slot(g * nb + b)
        toks = pl.ds(pl.multiple_of(b * L, L), L)
        cs, dtb = cs_ref[:, toks], dt_ref[:, toks]
        cst = jnp.transpose(cs)
        gram_b = gram[b]
        dg = jnp.zeros((L, L), F32)
        for j in range(HG):
            xj, dyj = x_ref[j, :, toks], dy_ref[j, :, toks]
            e = jnp.exp2(jnp.where(below, jnp.broadcast_to(cst[:, j:j + 1], (L, L)) - cs[j:j + 1], NEG))
            mhi, mlo = split(gram_b * e)
            dui_ref[j, :, toks] = dot(jnp.concatenate([dyj, dyj], axis=1), jnp.concatenate([mhi, mlo], axis=0))
            w = dot(dyj, xj, TN) * (e * dtb[j:j + 1])
            dg = dg + w
            rsum[:, (2 * j) * L:(2 * j + 1) * L], rsum[:, (2 * j + 1) * L:(2 * j + 2) * L] = split(w * gram_b)
        dg_ref[b] += dg
        rs_ref[:, toks] = jnp.transpose(dot(rsum[...], pick[...]))[:HG]
        return 0

    lax.fori_loop(0, nb, work, 0)

    @pl.when(g == pl.num_programs(0) - 1)
    def _():
        def rest(n, _):
            slot(n)
            return 0

        lax.fori_loop((H // HG) * nb, max(HOP * (ng - 1) + BACK, HOP * (ng - 1) + F_HOP * (ng // 2) + 1 + F_BACK) + QH, rest, 0)

        def drain(k, _):
            for d in range(2):
                x_copy(d, k).wait_send()
                b_copy(d, k).wait_send()

                @pl.when((pos < ng - 1) if d == 0 else (pos > 0))
                def _():
                    c_copy(d, k).wait_send()

                for i in range(2):
                    d_copy(d, i, k).wait()

            for way in range(2):
                @pl.when(f_sends[way])
                def _():
                    f_copy(way, k).wait_send()

            fx_copy(k).wait_send()
            for i in range(2):
                fd_copy(i, k).wait()
            return 0

        early = [pltpu.make_async_copy(fq, first_ref.at[rows(QH * q, QH)], out_sem.at[2]),
                 pltpu.make_async_copy(fxr, first_ref.at[rows(QH * oq, QH)], out_sem.at[3])]
        for out in early:
            out.start()
        lax.fori_loop(0, QH, drain, 0)
        outs = [pltpu.make_async_copy(into.at[0], s_end, out_sem.at[0]), pltpu.make_async_copy(into.at[1], g_end, out_sem.at[1])]
        for out in outs:
            out.start()
        for o in range(1, GD):
            tot_copy(o).wait_send()
        for d in range(2):
            for i in range(2):
                par_copy(d, i).wait_send()
        for out in early + outs:
            out.wait()


def chain_and_blocks(nd, x, dy, dt, cs, b, c, tot, s_loc, g_loc, s0, g0):
    t = x.shape[2]
    nb = t // L
    full = lambda shape: pl.BlockSpec(shape, lambda g: (0,) * len(shape))
    heads = pl.BlockSpec((HG, PD, t), lambda g: (g, 0, 0))
    rows = pl.BlockSpec((HG, t), lambda g: (g, 0))
    anywhere = pl.BlockSpec(memory_space=pl.ANY)
    quarter = pltpu.VMEM((2, QR, N), F32)
    whole = pltpu.VMEM((2, H * PD, N), F32)
    halves = pltpu.VMEM((2, 2, QR, N), F32)
    sems = lambda *shape: pltpu.SemaphoreType.DMA(shape)
    state = jax.ShapeDtypeStruct((H * PD, N), F32)
    return pl.pallas_call(
        functools.partial(chain_kernel, nd),
        grid=(H // HG,),
        in_specs=[heads, heads, rows, rows, full((t, N)), full((t, N))] + [anywhere] * 5,
        out_specs=[heads, rows, full((nb, L, L)), anywhere, anywhere, anywhere],
        out_shape=[jax.ShapeDtypeStruct((H, PD, t), F32), jax.ShapeDtypeStruct((H, t), F32), jax.ShapeDtypeStruct((nb, L, L), F32), state, state, state],
        scratch_shapes=[pltpu.VMEM((nb, L, L), F32), pltpu.VMEM((GD, H, L), F32), whole, halves] + [quarter] * 7 + [halves, whole, pltpu.VMEM((L, 2 * HG * L), BF16), pltpu.VMEM((2 * HG * L, L), BF16),
                           pltpu.VMEM((QR, N), F32), pltpu.VMEM((QR, N), F32)]
                       + [sems(5), sems(GD), sems(GD), sems(2, 2), sems(2, 2)] + [sems(2, QH)] * 6 + [sems(2, 2, QH)] * 2 + [sems(2, QH)] + [sems(QH)] * 3 + [sems(2, QH)] * 2 + [sems(4)],
        compiler_params=pltpu.CompilerParams(dimension_semantics=("arbitrary",), collective_id=0, has_side_effects=True),
        cost_estimate=pl.CostEstimate(flops=10 ** 10, bytes_accessed=10 ** 7, transcendentals=0),
        name="chain_and_blocks",
    )(x, dy, dt, cs, b, c, tot, s_loc, g_loc, s0, g0)


def carried_kernel(x_ref, dy_ref, dt_ref, cs_ref, dui_ref, rs_ref, s0_ref, g1_ref, b_ref, c_ref, par_ref, dta_ref, para_ref, dg_ref,
                   dx_ref, ddt_ref, db_ref, dc_ref, dh_ref,
                   sf, gc, tu, sd, gh, us, db_acc, dc_acc, ec_s, td_s, tl_s, ddir_s, xd_s, dcs_s, kd_s, bb_ref, cc_ref, b2t_ref, ct_ref):
    nb = x_ref.shape[2] // L
    g = pl.program_id(0)

    @pl.when(g == 0)
    def _():
        for b in range(nb):
            bb, cc = b_ref[b * L:(b + 1) * L, :], c_ref[b * L:(b + 1) * L, :]
            bb_ref[b] = jnp.concatenate([bb, bb], axis=0)
            cc_ref[b] = jnp.concatenate([cc, cc], axis=0)
            bt = jnp.transpose(bb.astype(F32)).astype(BF16)
            b2t_ref[b] = jnp.concatenate([bt, bt], axis=0)
            ct_ref[b] = jnp.transpose(cc.astype(F32))
        db_acc[...] = jnp.zeros_like(db_acc)
        dc_acc[...] = jnp.zeros_like(dc_acc)

    heads = pl.ds(pl.multiple_of(g * HG, HG), HG)
    for b in range(nb):
        sl = slice(b * L, (b + 1) * L)
        cs = cs_ref[:, sl]
        tail = jnp.exp2(cs[:, L - 1:L] - cs)
        ec_s[b] = jnp.exp2(cs)
        tl_s[b] = tail
        td_s[b] = tail * dt_ref[:, sl]

    sf[0] = s0_ref[...]

    def forward(b, _):
        toks = pl.ds(pl.multiple_of(b * L, L), L)
        etot = ec_s[b][:, L - 1:L]
        td = td_s[b]
        for j in range(HG):
            hi, lo = split(x_ref[j, :, toks].astype(F32) * td[j:j + 1])
            tu[b, j * PD:(j + 1) * PD, :L] = hi
            tu[b, j * PD:(j + 1) * PD, L:] = lo
        new = dot(tu[b], bb_ref[b])
        for j in range(HG):
            pr = slice(j * PD, (j + 1) * PD)
            sf[b + 1, pr] = etot[j:j + 1] * sf[b, pr] + new[pr]
        return 0

    lax.fori_loop(0, nb, forward, 0)
    gc[...] = g1_ref[...]

    def backward(i, _):
        b = nb - 1 - i
        toks = pl.ds(pl.multiple_of(b * L, L), L)
        ec, tl, dtb = ec_s[b], tl_s[b], dt_ref[:, toks]
        etot = ec[:, L - 1:L]
        kd = []
        for j in range(HG):
            pr = slice(j * PD, (j + 1) * PD)
            gj = gc[pr]
            kd.append(jnp.sum(gj * sf[b + 1, pr], axis=0, keepdims=True))
            hi, lo = split(gj)
            gh[pr, :L] = hi
            gh[pr, L:] = lo
            hi, lo = split(dy_ref[j, :, toks].astype(F32) * ec[j:j + 1])
            sd[pr, :L] = hi
            sd[pr, L:] = lo
        kd_s[b, heads] = jnp.concatenate(kd, axis=0)
        us[...] = dot(gh[...], b2t_ref[b])
        wide = dot(gh[...], tu[b], TN)
        db_acc[b] += (wide[:N, :L] + wide[:N, L:]) + (wide[N:, :L] + wide[N:, L:])
        ct = ct_ref[b]
        dc = jnp.zeros((N, L), F32)
        ddir, xd, inter = [], [], []
        for j in range(HG):
            pr = slice(j * PD, (j + 1) * PD)
            du = dui_ref[j, :, toks] + us[pr] * tl[j:j + 1]
            xf, dyf = x_ref[j, :, toks].astype(F32), dy_ref[j, :, toks].astype(F32)
            ddir.append(jnp.sum(du * xf, axis=0, keepdims=True))
            xd.append(jnp.sum(dyf * xf, axis=0, keepdims=True))
            dx_ref[j, :, toks] = (du * dtb[j:j + 1] + dyf * par_ref[j:j + 1, 1:2]).astype(BF16)
            shi, slo = split(sf[b, pr])
            st = jnp.transpose(jnp.concatenate([shi, slo], axis=0))
            st = jnp.concatenate([st, st], axis=1)
            dhi, dlo = sd[pr, :L], sd[pr, L:]
            z = dot(st, jnp.concatenate([dhi, dhi, dlo, dlo], axis=0))
            dc = dc + z
            inter.append(jnp.sum(z * ct, axis=0, keepdims=True))
        dc_acc[b] += dc
        ddir = jnp.concatenate(ddir, axis=0)
        ddir_s[b, heads] = ddir
        xd_s[b, heads] = jnp.concatenate(xd, axis=0)
        dcs_s[b, heads] = rs_ref[:, toks] + jnp.concatenate(inter, axis=0) - ddir * dtb
        grow = dot(sd[...], cc_ref[b])
        for j in range(HG):
            pr = slice(j * PD, (j + 1) * PD)
            gc[pr] = etot[j:j + 1] * gc[pr] + grow[pr]
        return 0

    lax.fori_loop(0, nb, backward, 0)

    @pl.when(g == pl.num_programs(0) - 1)
    def _():
        after = (lax.broadcasted_iota(jnp.int32, (L, L), 0) >= lax.broadcasted_iota(jnp.int32, (L, L), 1)).astype(F32)
        da_sum = jnp.zeros((H, 1), F32)
        dd_sum = jnp.zeros((H, 1), F32)
        for b in range(nb):
            sl = slice(b * L, (b + 1) * L)
            da = dot(dcs_s[b], after, precision=HIGHEST) + jnp.sum(kd_s[b], axis=1, keepdims=True)
            dta = da * para_ref[:, 0:1]
            ddt_ref[:, sl] = ddir_s[b] + dta
            da_sum += jnp.sum(dta * dta_ref[:, sl], axis=1, keepdims=True)
            dd_sum += jnp.sum(xd_s[b], axis=1, keepdims=True)
            ghi, glo = split(dg_ref[b])
            dbt = jnp.transpose(db_acc[b]) + (dot(ghi, cc_ref[b, :L, :], TN) + dot(glo, cc_ref[b, :L, :], TN))
            dct = jnp.transpose(dc_acc[b]) + (dot(ghi, bb_ref[b, :L, :]) + dot(glo, bb_ref[b, :L, :]))
            db_ref[sl, :] = dbt.astype(BF16)
            dc_ref[sl, :] = dct.astype(BF16)
        lane_h = lax.broadcasted_iota(jnp.int32, (H, L), 1)
        dh_ref[...] = jnp.where(lane_h == 0, da_sum, jnp.where(lane_h == 1, dd_sum, 0.0))


def carried(x, dy, dt, cs, dui, rs, s_start, ds_end, b, c, par, dg):
    t = x.shape[2]
    nb = t // L
    full = lambda shape: pl.BlockSpec(shape, lambda g: (0,) * len(shape))
    heads = pl.BlockSpec((HG, PD, t), lambda g: (g, 0, 0))
    rows = pl.BlockSpec((HG, t), lambda g: (g, 0))
    state = pl.BlockSpec((HG * PD, N), lambda g: (g, 0))
    one = pl.BlockSpec((HG, L), lambda g: (g, 0))
    vm = lambda shape, dtype=F32: pltpu.VMEM(shape, dtype)
    return pl.pallas_call(
        carried_kernel,
        grid=(H // HG,),
        in_specs=[heads, heads, rows, rows, heads, rows, state, state, full((t, N)), full((t, N)), one, full((H, t)), full((H, L)),
                  full((nb, L, L))],
        out_specs=[heads, full((H, t)), full((t, N)), full((t, N)), full((H, L))],
        out_shape=[jax.ShapeDtypeStruct((H, PD, t), BF16), jax.ShapeDtypeStruct((H, t), F32), jax.ShapeDtypeStruct((t, N), BF16),
                   jax.ShapeDtypeStruct((t, N), BF16), jax.ShapeDtypeStruct((H, L), F32)],
        scratch_shapes=[vm((nb + 1, HG * PD, N)), vm((HG * PD, N)), vm((nb, HG * PD, 2 * L), BF16), vm((HG * PD, 2 * L), BF16),
                        vm((HG * PD, 2 * N), BF16), vm((HG * PD, L)), vm((nb, N, L)), vm((nb, N, L)),
                        vm((nb, HG, L)), vm((nb, HG, L)), vm((nb, HG, L)), vm((nb, H, L)), vm((nb, H, L)), vm((nb, H, L)), vm((nb, H, N)),
                        vm((nb, 2 * L, N), BF16), vm((nb, 2 * L, N), BF16), vm((nb, 2 * N, L), BF16), vm((nb, N, L))],
        compiler_params=pltpu.CompilerParams(dimension_semantics=("arbitrary",)),
        cost_estimate=pl.CostEstimate(flops=5 * 10 ** 10, bytes_accessed=6 * H * PD * t, transcendentals=H * t * L),
        name="carried_backward",
    )(x, dy, dt, cs, dui, rs, s_start, ds_end, b, c, par, dt, par, dg)


def solution(mesh):
    nd = mesh.shape[AXIS]
    tok4 = P(None, AXIS, None, None)
    tok3 = P(None, AXIS, None)

    def device_step(x_loc, dt_loc, a_log, b_loc, c_loc, d_skip, s_init, dy_loc, ds_last):
        x, dy = jnp.transpose(x_loc[0], (1, 2, 0)), jnp.transpose(dy_loc[0], (1, 2, 0))
        dt = jnp.transpose(dt_loc[0])
        b, c = b_loc[0], c_loc[0]
        col = jnp.arange(L)[None, :]
        par = jnp.where(col == 0, -jnp.exp(a_log)[:, None], jnp.where(col == 1, d_skip[:, None], 0.0))
        s_loc, g_loc, cs, tot = summaries(x, dy, dt, par, b, c)
        s0, g0 = s_init.reshape(H * PD, N), ds_last.reshape(H * PD, N)
        dui, rs, dg, s_start, ds_end, first = chain_and_blocks(nd, x, dy, dt, cs, b, c, tot, s_loc, g_loc, s0, g0)
        dx, ddt, db, dc, dh = carried(x, dy, dt, cs, dui, rs, s_start, ds_end, b, c, par, dg)
        dh = tile_sum(nd, dh)
        return (jnp.transpose(dx, (2, 0, 1))[None], jnp.transpose(ddt)[None], db[None], dc[None], first.reshape(1, H, PD, N), dh[0, :H], dh[1, :H])

    return jax.shard_map(device_step, mesh=mesh,
                         in_specs=(tok4, tok3, P(), tok3, tok3, P(), P(), tok4, P()),
                         out_specs=(tok4, tok3, tok3, tok3, P(), P(), P()),
                         check_vma=False)
```
